256 devices in a mesh: mode: 16 (over y_hi, z), sx: 4 (over x), sy: 4 (over y_lo, core).
Axes of the slice: x: 4, y: 4 (y_hi: 2, y_lo: 2; y = y_hi * 2 + y_lo), z: 8, core: 2. Of those that a mesh axis runs over, the one named last changes fastest.
Arguments:
- start_field: float32 [2048, 16, 512], P('mode', 'sx', 'sy'), may hold values from -2.5 to 2.5
- right_side: float32 [2048, 16, 512], P('mode', 'sx', 'sy'), may hold values from -6 to 6
- mean_coef: float32 [16, 512], P('sx', 'sy'), may hold values from 0.5 to 2
- term_coef: float32 [8, 16, 512], P(None, 'sx', 'sy'), may hold values from -3 to 3
- coupling: float32 [8, 2048, 2048], P(None, None, 'mode'), may hold values from -0.05 to 0.05, as said below
- block_mask: int32 [8, 16, 16], replicated, may hold values from 0 to 1, as said below
Outputs:
- solution: float32 [2048, 16, 512], P('mode', 'sx', 'sy')
- residual: float32 [2048, 16, 512], P('mode', 'sx', 'sy')
The draws below stay inside these ranges and needn't reach their ends.
Inputs may be any that keep to these rules, and one draw needn't show every extreme that they name: coupling[t] is symmetric: coupling[t, i, j] = coupling[t, j, i]. block_mask[t] is symmetric; entry [t, a, b] covers modes a * 128 to (a + 1) * 128 - 1 against b * 128 to (b + 1) * 128 - 1.
All inputs are finite; a program needn't handle non-finite values.
Results may differ from the reference program's by a relative error of at most 0.0002.
Values sent between devices are 32-bit elements; how exact they have to be, the bound alone decides.
A program may use at most 128 MiB of HBM per device.

```python
import math
import jax
import jax.numpy as jnp
from jax import lax

MODES = 2048
TERMS = 8
BLOCK = 128
SWEEPS = 3
OUTER = 1
NBLK = 16
NX = 16
NY = 512


def draw_coupling(key, part):
    subkey = jax.random.fold_in(key, 11)
    raw = jax.random.uniform(subkey, (TERMS, MODES, MODES), jnp.float32, -1.0, 1.0)
    return 0.025 * (raw + jnp.swapaxes(raw, 1, 2))


def draw_block_mask(key, part):
    subkey = jax.random.fold_in(key, 23)
    pattern = jax.random.randint(subkey, (TERMS, NBLK, NBLK), 0, 2).astype(jnp.int32)
    row_index = lax.broadcasted_iota(jnp.int32, (TERMS, NBLK, NBLK), 1)
    col_index = lax.broadcasted_iota(jnp.int32, (TERMS, NBLK, NBLK), 2)
    return jnp.where(row_index <= col_index, pattern, jnp.swapaxes(pattern, 1, 2)).astype(jnp.int32)


def block_levels(stream_key, shape, cuts, least, top_value):
    loudness = 1.0
    for dim, shards_of in cuts:
        steps = jax.random.uniform(jax.random.fold_in(jax.random.fold_in(stream_key, 6), dim), (shards_of,), jnp.float32, least / len(cuts), top_value / len(cuts))
        loudness = loudness * jnp.repeat(jnp.exp(steps), shape[dim] // shards_of).reshape((-1,) + (1,) * (len(shape) - 1 - dim))
    return loudness


def normal_values(stream_key, dims, scale, limit, split=(), kind=jnp.bfloat16):
    values = jax.random.normal(stream_key, dims, jnp.float32) * scale
    if len(split) > 0:
        values = block_levels(stream_key, dims, split, -0.22, 0.18) * values
    return jnp.clip(values, min=-limit, max=limit).astype(kind)


def setup_inputs(seed: int = 0) -> dict:
    seeds = jax.random.split(jax.random.key(seed), 7)
    return {
        "start_field": normal_values(seeds[0], (MODES, NX, NY), 0.3, 2.5, ((0, 16), (1, 4), (2, 4)), jnp.float32),
        "right_side": normal_values(seeds[1], (MODES, NX, NY), 1.0, 6.0, ((0, 16), (1, 4), (2, 4)), jnp.float32),
        "mean_coef": jnp.clip(jnp.exp(math.log(2.0) - 1.3862944 * jax.random.uniform(seeds[2], (NX, NY), jnp.float32) ** block_levels(seeds[2], (NX, NY), ((0, 4), (1, 4)), -0.2, 0.2)), 0.5, 2.0),
        "term_coef": normal_values(seeds[3], (TERMS, NX, NY), 0.5, 3.0, ((1, 4), (2, 4)), jnp.float32),
        "coupling": draw_coupling(jax.random.fold_in(seeds[6], 71), 0),
        "block_mask": draw_block_mask(jax.random.fold_in(seeds[6], 71), 0),
    }


react = 0.5
theta = 8.5
delta = 8.0


def flux(coef, values):
    total = jnp.zeros(values.shape, jnp.float32)
    for axis in (-2, -1):
        for shift in (1, -1):
            neigh_coef = jnp.roll(coef, shift, axis)
            neigh_val = jnp.roll(values, shift, axis)
            total = total + 0.5 * (coef + neigh_coef) * (values - neigh_val)
    return total


def mean_op(mean_coef, values):
    return flux(mean_coef, values) + react * values


def reference(start_field, right_side, mean_coef, term_coef, coupling, block_mask):
    field = start_field
    sigma = theta / delta
    residual = right_side
    for outer_step in range(OUTER):
        applied = mean_op(mean_coef, field)
        for term in range(TERMS):
            expanded = jnp.repeat(jnp.repeat(block_mask[term], BLOCK, 0), BLOCK, 1).astype(jnp.float32)
            masked = coupling[term] * expanded
            fluxes = flux(term_coef[term], field).reshape(MODES, -1)
            mixed = jnp.dot(masked, fluxes, precision=lax.Precision.HIGHEST)
            applied = applied + mixed.reshape(field.shape)
        residual = right_side - applied
        correction = jnp.zeros(field.shape, jnp.float32)
        direction = residual / theta
        rho = 1.0 / sigma
        for sweep in range(SWEEPS + 1):
            correction = correction + direction
            if sweep < SWEEPS:
                misfit = residual - mean_op(mean_coef, correction)
                rho_next = 1.0 / (2.0 * sigma - rho)
                direction = (rho_next * rho) * direction + (2.0 * rho_next / delta) * misfit
                rho = rho_next
        field = field + correction
    return field, residual
```

```python
import jax
import jax.numpy as jnp
from jax import lax
from jax.sharding import PartitionSpec as P

SWEEPS = 3


react = 0.5
theta = 8.5
delta = 8.0


def extended(value, sides, width):
    for axis, dim in sides:
        devices, length = (lax.axis_size(axis), value.shape[dim])
        up = [(i, (i + 1) % devices) for i in range(devices)]
        down = [(j, i) for i, j in up]
        last = lax.slice_in_dim(value, length - width, length, axis=dim)
        initial = lax.slice_in_dim(value, 0, width, axis=dim)
        before = lax.ppermute(last, axis, up)
        after = lax.ppermute(initial, axis, down)
        value = jnp.concatenate([before, value, after], axis=dim)
    return value


def crop(values, margin):
    return values[..., margin:-margin, margin:-margin]


def flux_pad(coef, padded):
    width_x = padded.shape[-2] - 2
    width_y = padded.shape[-1] - 2
    center_coef = coef[..., 1:-1, 1:-1]
    center_val = padded[..., 1:-1, 1:-1]
    total = None
    for off_x, off_y in ((0, 1), (2, 1), (1, 0), (1, 2)):
        neigh_coef = coef[..., off_x : off_x + width_x, off_y : off_y + width_y]
        neigh_val = padded[..., off_x : off_x + width_x, off_y : off_y + width_y]
        term_value = 0.5 * (center_coef + neigh_coef) * (center_val - neigh_val)
        total = term_value if total is None else total + term_value
    return total


def local(start_field, right_side, mean_coef, term_coef, coupling, block_mask):
    mode_rows = start_field.shape[0]
    term_count = coupling.shape[0]
    total_modes = coupling.shape[1]
    block_count = block_mask.shape[1]
    block_size = total_modes // block_count
    sigma = theta / delta
    stacked = jnp.concatenate([mean_coef[None], term_coef], 0)
    coef_pad = extended(stacked, (("sx", 1), ("sy", 2)), SWEEPS)
    coef_one = crop(coef_pad, SWEEPS - 1)
    columns = lax.axis_index("mode") * mode_rows + jnp.arange(mode_rows, dtype=jnp.int32)
    selector = (
        jnp.arange(block_count, dtype=jnp.int32)[:, None] == (columns // block_size)[None, :]
    ).astype(jnp.float32)
    mask_cols = jnp.einsum(
        "tab,bj->taj", block_mask.astype(jnp.float32), selector, precision=lax.Precision.HIGHEST
    )
    masked = (
        coupling.reshape(term_count, block_count, block_size, mode_rows) * mask_cols[:, :, None, :]
    ).reshape(term_count, total_modes, mode_rows)
    field = start_field
    padded_field = extended(field, (("sx", 1), ("sy", 2)), 1)
    applied = flux_pad(coef_one[0], padded_field) + react * field
    cells = field.shape[1] * field.shape[2]
    fluxes = flux_pad(coef_one[1:, None], padded_field[None]).reshape(term_count, mode_rows, cells)
    partial = jnp.einsum("tij,tjc->ic", masked, fluxes, precision=lax.Precision.HIGH)
    coupled = lax.psum_scatter(partial, "mode", scatter_dimension=0, tiled=True).reshape(field.shape)
    residual = right_side - (applied + coupled)
    rho = 1.0 / sigma
    correction = jnp.zeros(residual.shape, jnp.float32)
    direction = residual / theta
    for sweep in range(SWEEPS + 1):
        correction = correction + direction
        if sweep < SWEEPS:
            padded_corr = extended(correction, (("sx", 1), ("sy", 2)), 1)
            misfit = residual - (flux_pad(coef_one[0], padded_corr) + react * correction)
            rho_next = 1.0 / (2.0 * sigma - rho)
            direction = rho_next * rho * direction + 2.0 * rho_next / delta * misfit
            rho = rho_next
    field = field + correction
    return (field, residual)


def solution(mesh):
    placed = (
        P("mode", "sx", "sy"),
        P("mode", "sx", "sy"),
        P("sx", "sy"),
        P(None, "sx", "sy"),
        P(None, None, "mode"),
        P(),
    )
    return jax.shard_map(
        local,
        mesh=mesh,
        in_specs=placed,
        out_specs=(P("mode", "sx", "sy"), P("mode", "sx", "sy")),
        check_vma=False,
    )
```

```python
import functools

import jax
import jax.numpy as jnp
from jax import lax
from jax.experimental import pallas as pl
from jax.experimental.pallas import tpu as pltpu
from jax.sharding import PartitionSpec as P

SWEEPS = 3
REACT = 0.5
THETA = 8.5
DELTA = 8.0
MESH = pl.DeviceIdType.MESH
RING = 8
GROUPS = 2
ROWS = 128
HALF = 64
WIDE = 4
LANES = 128
CELLS = WIDE * LANES
TERMS = 8

UNITS = ((0, 0, HALF, 1), (0, HALF, HALF, -1), (1, 0, HALF, 1), (1, HALF, HALF, -1))


def hops(unit, way):
    return 4 if UNITS[unit][3] == way else 3


def orders():
    lead = [(0, 4), (1, 3), (0, 3), (1, 2), (0, 2), (1, 1), (0, 1)]
    tail = [(u + 2, o) for u, o in lead]
    picks = "aabaabaaabbbbb"
    both = {"a": iter(lead), "b": iter(tail)}
    plus = [next(both[c]) for c in picks]
    minus = [(u ^ 1, o) for u, o in plus]
    return plus, minus


PLUS, MINUS = orders()
INBOX = {}
for way_, order_ in ((1, PLUS), (-1, MINUS)):
    for u_, o_ in order_:
        INBOX[(way_, u_, o_ - 1)] = len(INBOX)


def kernel(
    field, right, mean, terms, coupling, mask, sol, res,
    abuf, lhs_hi, lhs_lo, f_hi, f_lo, part, inbox, ysum, ybox,
    vp, diffs, base, coef, cbox, kd, resid, corr, edge, rowbox, colbox,
    asem, csend, crecv, hsend, hrecv, rsend, rrecv, ysend, yrecv,
):
    mode = lax.axis_index("mode")
    sx = lax.axis_index("sx")
    sy = lax.axis_index("sy")
    z = lax.rem(mode, RING)
    group = lax.div(mode, RING)
    nx, ny = 4, 4
    zp = (group * RING + lax.rem(z + 1, RING), sx, sy)
    zm = (group * RING + lax.rem(z + RING - 1, RING), sx, sy)
    partner = (lax.rem(mode + RING, 2 * RING), sx, sy)
    xp = (mode, lax.rem(sx + 1, nx), sy)
    xm = (mode, lax.rem(sx + nx - 1, nx), sy)
    yp = (mode, sx, lax.rem(sy + 1, ny))
    ym = (mode, sx, lax.rem(sy + ny - 1, ny))

    barrier = pltpu.get_barrier_semaphore()
    peers = (zp, zm, partner, xp, xm, yp, ym)
    for peer in peers:
        pl.semaphore_signal(barrier, inc=1, device_id=peer, device_id_type=MESH)

    def block_of(o, p):
        owner = group if p == 1 else 1 - group
        return owner * RING + lax.rem(z + o, RING)

    def load(o, p):
        row = pl.multiple_of(block_of(o, p) * ROWS, ROWS)
        return pltpu.make_async_copy(
            coupling.at[:, pl.ds(row, ROWS), :], abuf.at[o * 2 + p], asem.at[o * 2 + p]
        )

    for o in (4, 3, 5, 2, 6, 1, 0, 7):
        for p in (0, 1):
            load(o, p).start()

    lane = lax.broadcasted_iota(jnp.int32, (ROWS, LANES), 1)

    def edges(planes, slot):
        low, high = None, None
        for x in range(WIDE):
            lo_x = planes[x] if x == 0 else pltpu.roll(planes[x], x, 1)
            hi_x = pltpu.roll(planes[x], x + 1, 1)
            low = lo_x if x == 0 else jnp.where(lane == x, lo_x, low)
            high = hi_x if x == 0 else jnp.where(lane == x, hi_x, high)
        edge[slot, 0] = low
        edge[slot, 1] = high

    started = []

    def send(src, dst, ssem, rsem, peer):
        copy = pltpu.make_async_remote_copy(
            src_ref=src, dst_ref=dst, send_sem=ssem, recv_sem=rsem, device_id=peer, device_id_type=MESH
        )
        copy.start()
        started.append(copy)
        return copy

    def swap(slot, first, last):
        return [
            send(last, rowbox.at[slot, 0], hsend.at[slot, 0], hrecv.at[slot, 0], xp),
            send(first, rowbox.at[slot, 1], hsend.at[slot, 1], hrecv.at[slot, 1], xm),
            send(edge.at[slot, 1], colbox.at[slot, 0], hsend.at[slot, 2], hrecv.at[slot, 2], yp),
            send(edge.at[slot, 0], colbox.at[slot, 1], hsend.at[slot, 3], hrecv.at[slot, 3], ym),
        ]

    def differences(planes, slot, x):
        center = planes(x)
        up = planes(x - 1) if x > 0 else rowbox[slot, 0]
        down = planes(x + 1) if x < WIDE - 1 else rowbox[slot, 1]
        lo_col = colbox[slot, 0] if x == 0 else pltpu.roll(colbox[slot, 0], LANES - x, 1)
        hi_col = pltpu.roll(colbox[slot, 1], LANES - 1 - x, 1)
        left = jnp.where(lane == 0, lo_col, pltpu.roll(center, 1, 1))
        after = jnp.where(lane == LANES - 1, hi_col, pltpu.roll(center, LANES - 1, 1))
        return center, (center - up, center - down, center - left, center - after)

    values = []
    for x in range(WIDE):
        plane = field[pl.ds(x, ROWS, stride=WIDE), :]
        vp[x] = plane
        values.append(plane)
    edges(values, 0)
    for x in range(WIDE):
        coef[x, 0:TERMS, :] = terms[pl.ds(x, TERMS, stride=WIDE), :]
        coef[x, TERMS : 2 * TERMS, :] = jnp.broadcast_to(mean[x : x + 1, :], (TERMS, LANES))

    pl.semaphore_wait(barrier, len(peers))

    coefs = [
        send(coef, cbox.at[0], csend.at[0], crecv.at[0], xp),
        send(coef, cbox.at[1], csend.at[1], crecv.at[1], xm),
        send(coef, cbox.at[2], csend.at[2], crecv.at[2], yp),
        send(coef, cbox.at[3], csend.at[3], crecv.at[3], ym),
    ]
    halo = swap(0, vp.at[0], vp.at[WIDE - 1])

    def prepare(o):
        for p in (0, 1):
            load(o, p).wait()
            blk = block_of(o, p)
            for t in range(TERMS):
                value = abuf[o * 2 + p, t] * mask[t, blk, mode].astype(jnp.float32)
                high = value.astype(jnp.bfloat16)
                low = (value - high.astype(jnp.float32)).astype(jnp.bfloat16)
                lhs_hi[p * ROWS : (p + 1) * ROWS, t * ROWS : (t + 1) * ROWS] = high
                lhs_lo[p * ROWS : (p + 1) * ROWS, t * ROWS : (t + 1) * ROWS] = low

    def multiply(o):
        for n in range(2):
            cols = slice(n * 2 * LANES, (n + 1) * 2 * LANES)
            dot = functools.partial(jnp.dot, preferred_element_type=jnp.float32)
            total = (
                dot(lhs_hi[...], f_hi[:, cols])
                + dot(lhs_hi[...], f_lo[:, cols])
                + dot(lhs_lo[...], f_hi[:, cols])
            )
            part[o, 0, :, cols] = total[0:ROWS]
            part[o, 1, :, cols] = total[ROWS:]

    prepare(4)

    for copy in coefs:
        copy.wait_recv()
    thin = lax.broadcasted_iota(jnp.int32, (2 * TERMS, LANES), 1)
    for x in range(WIDE):
        here = coef[x]
        up = coef[x - 1] if x > 0 else cbox[0, WIDE - 1]
        down = coef[x + 1] if x < WIDE - 1 else cbox[1, 0]
        left = jnp.where(thin == 0, pltpu.roll(cbox[2, x], 1, 1), pltpu.roll(here, 1, 1))
        after = jnp.where(thin == LANES - 1, pltpu.roll(cbox[3, x], LANES - 1, 1), pltpu.roll(here, LANES - 1, 1))
        for d, other in enumerate((up, down, left, after)):
            kd[d, x] = 0.5 * (here + other)

    for copy in halo:
        copy.wait_recv()
    for x in range(WIDE):
        center, deltas = differences(lambda i: vp[i], 0, x)
        for d in range(4):
            diffs[d, x] = deltas[d]

    @pl.loop(0, TERMS)
    def _(t):
        rows = pl.ds(pl.multiple_of(t * ROWS, ROWS), ROWS)
        for x in range(WIDE):
            total = None
            for d in range(4):
                piece = kd[d, x, pl.ds(t, 1), :] * diffs[d, x]
                total = piece if total is None else total + piece
            high = total.astype(jnp.bfloat16)
            cols = slice(x * LANES, (x + 1) * LANES)
            f_hi[rows, cols] = high
            f_lo[rows, cols] = (total - high.astype(jnp.float32)).astype(jnp.bfloat16)

    multiply(4)

    ring = {}

    def forward(way, unit, o):
        p, first, count, _ = UNITS[unit]
        at = (o * way) % RING
        if o < hops(unit, way):
            ring[(way, unit, o)].wait_recv()
            part[at, p, first : first + count, :] += inbox[INBOX[(way, unit, o)]]
        i = INBOX[(way, unit, o - 1)]
        ring[(way, unit, o - 1)] = send(
            part.at[at, p, pl.ds(first, count), :],
            inbox.at[i],
            rsend.at[i],
            rrecv.at[i],
            zp if way == 1 else zm,
        )

    def collect(unit):
        p, first, count, _ = UNITS[unit]
        for way in (1, -1):
            ring[(way, unit, 0)].wait_recv()
        return (
            part[0, p, first : first + count, :]
            + inbox[INBOX[(1, unit, 0)]]
            + inbox[INBOX[(-1, unit, 0)]]
        )

    def several(count, pick):
        @pl.loop(0, count)
        def _(i):
            o = pick(i)
            prepare(o)
            multiply(o)

    swaps = []
    for slot, (one, two) in enumerate(zip(PLUS, MINUS)):
        if slot == 1:
            several(2, lambda i: 3 + 2 * i)
        if slot == 4:
            several(2, lambda i: 2 + 4 * i)
        if slot == 7:
            several(3, lambda i: lax.rem(1 + 7 * i, RING))
        forward(1, *one)
        forward(-1, *two)
        if slot == 8:
            for x in range(WIDE):
                total = REACT * vp[x]
                for d in range(4):
                    total = total + kd[d, x, TERMS : TERMS + 1, :] * diffs[d, x]
                base[x] = right[pl.ds(x, ROWS, stride=WIDE), :] - total
        if slot == 10:
            for unit in (0, 1):
                ysum[unit] = collect(unit)
                swaps.append(send(ysum.at[unit], ybox.at[unit], ysend.at[unit], yrecv.at[unit], partner))

    for unit in (2, 3):
        swaps[unit - 2].wait_recv()
        total = collect(unit) + ybox[unit - 2]
        rows = slice(UNITS[unit][1], UNITS[unit][1] + UNITS[unit][2])
        for x in range(WIDE):
            resid[x, rows, :] = base[x, rows, :] - total[:, x * LANES : (x + 1) * LANES]

    sigma = THETA / DELTA
    rho = 1.0 / sigma
    direction = []
    for x in range(WIDE):
        value = resid[x]
        res[pl.ds(x, ROWS, stride=WIDE), :] = value
        corr[0, x] = value / THETA
        diffs[0, x] = corr[0, x]
    for sweep in range(SWEEPS):
        edges([corr[sweep, x] for x in range(WIDE)], sweep + 1)
        moved = swap(sweep + 1, corr.at[sweep, 0], corr.at[sweep, WIDE - 1])
        for copy in moved:
            copy.wait_recv()
        rho_next = 1.0 / (2.0 * sigma - rho)
        for x in range(WIDE):
            center, deltas = differences(lambda i: corr[sweep, i], sweep + 1, x)
            applied = REACT * center
            for d in range(4):
                applied = applied + kd[d, x, TERMS : TERMS + 1, :] * deltas[d]
            misfit = resid[x] - applied
            step = rho_next * rho * diffs[0, x] + 2.0 * rho_next / DELTA * misfit
            if sweep < SWEEPS - 1:
                diffs[0, x] = step
                corr[sweep + 1, x] = center + step
            else:
                sol[pl.ds(x, ROWS, stride=WIDE), :] = vp[x] + (center + step)
        rho = rho_next

    for copy in started:
        copy.wait_send()


def local(start_field, right_side, mean_coef, term_coef, coupling, block_mask):
    modes, wide, lanes = start_field.shape
    f32, bf16 = jnp.float32, jnp.bfloat16
    vmem = pl.BlockSpec(memory_space=pltpu.VMEM)
    flat = jax.ShapeDtypeStruct((modes * wide, lanes), f32)
    sol, res = pl.pallas_call(
        kernel,
        out_shape=(flat, flat),
        in_specs=[
            vmem,
            vmem,
            vmem,
            vmem,
            pl.BlockSpec(memory_space=pl.ANY),
            pl.BlockSpec(memory_space=pltpu.SMEM),
        ],
        out_specs=(vmem, vmem),
        scratch_shapes=[
            pltpu.VMEM((2 * RING, TERMS, ROWS, ROWS), f32),
            pltpu.VMEM((2 * ROWS, TERMS * ROWS), bf16),
            pltpu.VMEM((2 * ROWS, TERMS * ROWS), bf16),
            pltpu.VMEM((TERMS * ROWS, CELLS), bf16),
            pltpu.VMEM((TERMS * ROWS, CELLS), bf16),
            pltpu.VMEM((RING, 2, ROWS, CELLS), f32),
            pltpu.VMEM((len(INBOX), HALF, CELLS), f32),
            pltpu.VMEM((2, HALF, CELLS), f32),
            pltpu.VMEM((2, HALF, CELLS), f32),
            pltpu.VMEM((WIDE, ROWS, LANES), f32),
            pltpu.VMEM((4, WIDE, ROWS, LANES), f32),
            pltpu.VMEM((WIDE, ROWS, LANES), f32),
            pltpu.VMEM((WIDE, 2 * TERMS, LANES), f32),
            pltpu.VMEM((4, WIDE, 2 * TERMS, LANES), f32),
            pltpu.VMEM((4, WIDE, 2 * TERMS, LANES), f32),
            pltpu.VMEM((WIDE, ROWS, LANES), f32),
            pltpu.VMEM((SWEEPS, WIDE, ROWS, LANES), f32),
            pltpu.VMEM((SWEEPS + 1, 2, ROWS, LANES), f32),
            pltpu.VMEM((SWEEPS + 1, 2, ROWS, LANES), f32),
            pltpu.VMEM((SWEEPS + 1, 2, ROWS, LANES), f32),
            pltpu.SemaphoreType.DMA((2 * RING,)),
            pltpu.SemaphoreType.DMA((4,)),
            pltpu.SemaphoreType.DMA((4,)),
            pltpu.SemaphoreType.DMA((SWEEPS + 1, 4)),
            pltpu.SemaphoreType.DMA((SWEEPS + 1, 4)),
            pltpu.SemaphoreType.DMA((len(INBOX),)),
            pltpu.SemaphoreType.DMA((len(INBOX),)),
            pltpu.SemaphoreType.DMA((2,)),
            pltpu.SemaphoreType.DMA((2,)),
        ],
        compiler_params=pltpu.CompilerParams(
            collective_id=0, has_side_effects=True, vmem_limit_bytes=48 * 1024 * 1024
        ),
        name="galerkin_step",
    )(
        start_field.reshape(modes * wide, lanes),
        right_side.reshape(modes * wide, lanes),
        mean_coef,
        term_coef.reshape(-1, lanes),
        coupling,
        block_mask,
    )
    return (sol.reshape(start_field.shape), res.reshape(start_field.shape))


def solution(mesh):
    placed = (
        P("mode", "sx", "sy"),
        P("mode", "sx", "sy"),
        P("sx", "sy"),
        P(None, "sx", "sy"),
        P(None, None, "mode"),
        P(),
    )
    return jax.shard_map(
        local,
        mesh=mesh,
        in_specs=placed,
        out_specs=(P("mode", "sx", "sy"), P("mode", "sx", "sy")),
        check_vma=False,
    )
```

```python
import functools

import jax
import jax.numpy as jnp
from jax import lax
from jax.experimental import pallas as pl
from jax.experimental.pallas import tpu as pltpu
from jax.sharding import PartitionSpec as P

SWEEPS = 3
REACT = 0.5
THETA = 8.5
DELTA = 8.0
MESH = pl.DeviceIdType.MESH
RING = 8
GROUPS = 2
ROWS = 128
HALF = 64
WIDE = 4
LANES = 128
CELLS = WIDE * LANES
TERMS = 8

QUARTER = 32
UNITS = tuple((p, r, QUARTER, way) for p, r in ((0, 0), (1, 0), (1, HALF)) for r, way in ((r, 1), (r + QUARTER, -1)))

PLAN = (
    ("m", 4), ("y", 4), ("z", 0, 4), ("m", 3), ("y", 3), ("z", 2, 4), ("m", 5), ("y", 5), ("z", 1, 3), ("m", 2),
    ("y", 2), ("z", 3, 3), ("m", 6), ("y", 6), ("m", 1), ("y", 1), ("z", 0, 3), ("m", 7), ("y", 7), ("z", 2, 3),
    ("m", 0), ("z", 4, 4), ("z", 1, 2), ("z", 3, 2), ("z", 0, 2), ("z", 5, 3), ("z", 4, 3), ("z", 1, 1), ("z", 2, 2),
    ("z", 0, 1), ("z", 5, 2), ("z", 4, 2), ("z", 3, 1), ("b",), ("z", 2, 1), ("s",), ("y", 0), ("z", 5, 1), ("z", 4, 1),
)


def hops(unit, way):
    return 4 if UNITS[unit][3] == way else 3


INBOX = {}
for step_ in PLAN:
    if step_[0] == "z":
        INBOX[(1, step_[1], step_[2] - 1)] = len(INBOX)
        INBOX[(-1, step_[1] ^ 1, step_[2] - 1)] = len(INBOX)


def kernel(
    field_in, right_in, mean_in, terms_in, coupling, mask_in, sol, res,
    field, right, mean, terms, mask,
    abuf, lhs_hi, lhs_lo, f_hi, f_lo, part, inbox, ysum, ybox, sbox,
    vp, diffs, base, coef, cbox, kd, resid, corr, edge, rowbox, colbox,
    isem, asem, csend, crecv, hsend, hrecv, rsend, rrecv, ysend, yrecv,
):
    mode = lax.axis_index("mode")
    sx = lax.axis_index("sx")
    sy = lax.axis_index("sy")
    z = lax.rem(mode, RING)
    group = lax.div(mode, RING)
    nx, ny = 4, 4
    zp = (group * RING + lax.rem(z + 1, RING), sx, sy)
    zm = (group * RING + lax.rem(z + RING - 1, RING), sx, sy)
    partner = (lax.rem(mode + RING, 2 * RING), sx, sy)
    xp = (mode, lax.rem(sx + 1, nx), sy)
    xm = (mode, lax.rem(sx + nx - 1, nx), sy)
    yp = (mode, sx, lax.rem(sy + 1, ny))
    ym = (mode, sx, lax.rem(sy + ny - 1, ny))

    barrier = pltpu.get_barrier_semaphore()
    peers = (zp, zm, partner, xp, xm, yp, ym)
    for peer in peers:
        pl.semaphore_signal(barrier, inc=1, device_id=peer, device_id_type=MESH)

    fetch = [
        pltpu.make_async_copy(src, dst, isem.at[i])
        for i, (src, dst) in enumerate(
            ((field_in, field), (mean_in, mean), (terms_in, terms), (mask_in, mask), (right_in, right))
        )
    ]
    for copy in fetch:
        copy.start()

    def block_of(o, p):
        owner = group if p == 1 else 1 - group
        return owner * RING + lax.rem(z + o, RING)

    def load(o, p):
        row = pl.multiple_of(block_of(o, p) * ROWS, ROWS)
        return pltpu.make_async_copy(
            coupling.at[:, pl.ds(row, ROWS), :], abuf.at[o * 2 + p], asem.at[o * 2 + p]
        )

    for o in (4, 3, 5, 2, 6, 1, 0, 7):
        for p in (0, 1):
            load(o, p).start()

    lane = lax.broadcasted_iota(jnp.int32, (ROWS, LANES), 1)

    def edges(planes, slot):
        low, high = None, None
        for x in range(WIDE):
            lo_x = planes[x] if x == 0 else pltpu.roll(planes[x], x, 1)
            hi_x = pltpu.roll(planes[x], x + 1, 1)
            low = lo_x if x == 0 else jnp.where(lane == x, lo_x, low)
            high = hi_x if x == 0 else jnp.where(lane == x, hi_x, high)
        edge[slot, 0] = low
        edge[slot, 1] = high

    started = []

    def send(src, dst, ssem, rsem, peer):
        copy = pltpu.make_async_remote_copy(
            src_ref=src, dst_ref=dst, send_sem=ssem, recv_sem=rsem, device_id=peer, device_id_type=MESH
        )
        copy.start()
        started.append(copy)
        return copy

    def swap(slot, first, last):
        return [
            send(last, rowbox.at[slot, 0], hsend.at[slot, 0], hrecv.at[slot, 0], xp),
            send(first, rowbox.at[slot, 1], hsend.at[slot, 1], hrecv.at[slot, 1], xm),
            send(edge.at[slot, 1], colbox.at[slot, 0], hsend.at[slot, 2], hrecv.at[slot, 2], yp),
            send(edge.at[slot, 0], colbox.at[slot, 1], hsend.at[slot, 3], hrecv.at[slot, 3], ym),
        ]

    def differences(planes, slot, x):
        center = planes(x)
        up = planes(x - 1) if x > 0 else rowbox[slot, 0]
        down = planes(x + 1) if x < WIDE - 1 else rowbox[slot, 1]
        lo_col = colbox[slot, 0] if x == 0 else pltpu.roll(colbox[slot, 0], LANES - x, 1)
        hi_col = pltpu.roll(colbox[slot, 1], LANES - 1 - x, 1)
        left = jnp.where(lane == 0, lo_col, pltpu.roll(center, 1, 1))
        after = jnp.where(lane == LANES - 1, hi_col, pltpu.roll(center, LANES - 1, 1))
        return center, (center - up, center - down, center - left, center - after)

    values = []
    fetch[0].wait()
    for x in range(WIDE):
        plane = field[pl.ds(x, ROWS, stride=WIDE), :]
        vp[x] = plane
        values.append(plane)
    edges(values, 0)
    fetch[1].wait()
    fetch[2].wait()
    for x in range(WIDE):
        coef[x, 0:TERMS, :] = terms[pl.ds(x, TERMS, stride=WIDE), :]
        coef[x, TERMS : 2 * TERMS, :] = jnp.broadcast_to(mean[x : x + 1, :], (TERMS, LANES))

    pl.semaphore_wait(barrier, len(peers))

    coefs = [
        send(coef, cbox.at[0], csend.at[0], crecv.at[0], xp),
        send(coef, cbox.at[1], csend.at[1], crecv.at[1], xm),
        send(coef, cbox.at[2], csend.at[2], crecv.at[2], yp),
        send(coef, cbox.at[3], csend.at[3], crecv.at[3], ym),
    ]
    halo = swap(0, vp.at[0], vp.at[WIDE - 1])

    def prepare(o):
        for p in (0, 1):
            load(o, p).wait()
            blk = block_of(o, p)
            for t in range(TERMS):
                value = abuf[o * 2 + p, t] * mask[t, blk, mode].astype(jnp.float32)
                high = value.astype(jnp.bfloat16)
                low = (value - high.astype(jnp.float32)).astype(jnp.bfloat16)
                lhs_hi[o, p * ROWS : (p + 1) * ROWS, t * ROWS : (t + 1) * ROWS] = high
                lhs_lo[o, p * ROWS : (p + 1) * ROWS, t * ROWS : (t + 1) * ROWS] = low

    def multiply(o):
        for n in range(2):
            cols = slice(n * 2 * LANES, (n + 1) * 2 * LANES)
            dot = functools.partial(jnp.dot, preferred_element_type=jnp.float32)
            total = (
                dot(lhs_hi[o], f_hi[:, cols])
                + dot(lhs_hi[o], f_lo[:, cols])
                + dot(lhs_lo[o], f_hi[:, cols])
            )
            part[o, 0, :, cols] = total[0:ROWS]
            part[o, 1, :, cols] = total[ROWS:]

    fetch[3].wait()
    prepare(4)

    for copy in coefs:
        copy.wait_recv()
    thin = lax.broadcasted_iota(jnp.int32, (2 * TERMS, LANES), 1)
    for x in range(WIDE):
        here = coef[x]
        up = coef[x - 1] if x > 0 else cbox[0, WIDE - 1]
        down = coef[x + 1] if x < WIDE - 1 else cbox[1, 0]
        left = jnp.where(thin == 0, pltpu.roll(cbox[2, x], 1, 1), pltpu.roll(here, 1, 1))
        after = jnp.where(thin == LANES - 1, pltpu.roll(cbox[3, x], LANES - 1, 1), pltpu.roll(here, LANES - 1, 1))
        for d, other in enumerate((up, down, left, after)):
            kd[d, x] = 0.5 * (here + other)

    for copy in halo:
        copy.wait_recv()
    for x in range(WIDE):
        center, deltas = differences(lambda i: vp[i], 0, x)
        for d in range(4):
            diffs[d, x] = deltas[d]

    @pl.loop(0, TERMS)
    def _(t):
        rows = pl.ds(pl.multiple_of(t * ROWS, ROWS), ROWS)
        for x in range(WIDE):
            total = None
            for d in range(4):
                piece = kd[d, x, pl.ds(t, 1), :] * diffs[d, x]
                total = piece if total is None else total + piece
            high = total.astype(jnp.bfloat16)
            cols = slice(x * LANES, (x + 1) * LANES)
            f_hi[rows, cols] = high
            f_lo[rows, cols] = (total - high.astype(jnp.float32)).astype(jnp.bfloat16)

    ring = {}
    crossing = {}
    crossed = set()

    def settle(o):
        if o not in crossed:
            crossed.add(o)
            crossing[o].wait_recv()
            part[o, 1, HALF:, :] += ybox[o]

    def forward(way, unit, o):
        p, first, count, _ = UNITS[unit]
        at = (o * way) % RING
        if unit >= 4:
            settle(at)
        if o < hops(unit, way):
            ring[(way, unit, o)].wait_recv()
            part[at, p, first : first + count, :] += inbox[INBOX[(way, unit, o)]]
        i = INBOX[(way, unit, o - 1)]
        ring[(way, unit, o - 1)] = send(
            part.at[at, p, pl.ds(first, count), :],
            inbox.at[i],
            rsend.at[i],
            rrecv.at[i],
            zp if way == 1 else zm,
        )

    def collect(unit):
        p, first, count, _ = UNITS[unit]
        for way in (1, -1):
            ring[(way, unit, 0)].wait_recv()
        return (
            part[0, p, first : first + count, :]
            + inbox[INBOX[(1, unit, 0)]]
            + inbox[INBOX[(-1, unit, 0)]]
        )

    sums = None
    for step in PLAN:
        if step[0] == "m":
            if step[1] != 4:
                prepare(step[1])
            multiply(step[1])
        elif step[0] == "z":
            forward(1, step[1], step[2])
            forward(-1, step[1] ^ 1, step[2])
        elif step[0] == "y":
            o = step[1]
            crossing[o] = send(
                part.at[o, 0, pl.ds(HALF, HALF), :], ybox.at[o], ysend.at[o], yrecv.at[o], partner
            )
        elif step[0] == "s":
            for unit in (0, 1):
                ysum[unit * QUARTER : (unit + 1) * QUARTER] = collect(unit)
            sums = send(ysum, sbox, ysend.at[RING], yrecv.at[RING], partner)
        else:
            fetch[4].wait()
            for x in range(WIDE):
                total = REACT * vp[x]
                for d in range(4):
                    total = total + kd[d, x, TERMS : TERMS + 1, :] * diffs[d, x]
                base[x] = right[pl.ds(x, ROWS, stride=WIDE), :] - total

    def finish(unit, extra):
        first = UNITS[unit][1]
        rows = slice(first, first + QUARTER)
        total = collect(unit)
        if extra is not None:
            total = total + extra
        for x in range(WIDE):
            resid[x, rows, :] = base[x, rows, :] - total[:, x * LANES : (x + 1) * LANES]

    sums.wait_recv()
    finish(2, sbox[0:QUARTER])
    finish(3, sbox[QUARTER:HALF])
    settle(0)
    finish(4, None)
    finish(5, None)

    sigma = THETA / DELTA
    rho = 1.0 / sigma
    direction = []
    for x in range(WIDE):
        value = resid[x]
        res[pl.ds(x, ROWS, stride=WIDE), :] = value
        corr[0, x] = value / THETA
        diffs[0, x] = corr[0, x]
    for sweep in range(SWEEPS):
        edges([corr[sweep, x] for x in range(WIDE)], sweep + 1)
        moved = swap(sweep + 1, corr.at[sweep, 0], corr.at[sweep, WIDE - 1])
        for copy in moved:
            copy.wait_recv()
        rho_next = 1.0 / (2.0 * sigma - rho)
        for x in range(WIDE):
            center, deltas = differences(lambda i: corr[sweep, i], sweep + 1, x)
            applied = REACT * center
            for d in range(4):
                applied = applied + kd[d, x, TERMS : TERMS + 1, :] * deltas[d]
            misfit = resid[x] - applied
            step = rho_next * rho * diffs[0, x] + 2.0 * rho_next / DELTA * misfit
            if sweep < SWEEPS - 1:
                diffs[0, x] = step
                corr[sweep + 1, x] = center + step
            else:
                sol[pl.ds(x, ROWS, stride=WIDE), :] = vp[x] + (center + step)
        rho = rho_next

    for copy in started:
        copy.wait_send()


def local(start_field, right_side, mean_coef, term_coef, coupling, block_mask):
    modes, wide, lanes = start_field.shape
    f32, bf16 = jnp.float32, jnp.bfloat16
    vmem = pl.BlockSpec(memory_space=pltpu.VMEM)
    flat = jax.ShapeDtypeStruct((modes * wide, lanes), f32)
    sol, res = pl.pallas_call(
        kernel,
        out_shape=(flat, flat),
        in_specs=[pl.BlockSpec(memory_space=pltpu.HBM)] * 6,
        out_specs=(vmem, vmem),
        scratch_shapes=[
            pltpu.VMEM((modes * wide, lanes), f32),
            pltpu.VMEM((modes * wide, lanes), f32),
            pltpu.VMEM(mean_coef.shape, f32),
            pltpu.VMEM((TERMS * WIDE, lanes), f32),
            pltpu.SMEM(block_mask.shape, jnp.int32),
            pltpu.VMEM((2 * RING, TERMS, ROWS, ROWS), f32),
            pltpu.VMEM((RING, 2 * ROWS, TERMS * ROWS), bf16),
            pltpu.VMEM((RING, 2 * ROWS, TERMS * ROWS), bf16),
            pltpu.VMEM((TERMS * ROWS, CELLS), bf16),
            pltpu.VMEM((TERMS * ROWS, CELLS), bf16),
            pltpu.VMEM((RING, 2, ROWS, CELLS), f32),
            pltpu.VMEM((len(INBOX), QUARTER, CELLS), f32),
            pltpu.VMEM((HALF, CELLS), f32),
            pltpu.VMEM((RING, HALF, CELLS), f32),
            pltpu.VMEM((HALF, CELLS), f32),
            pltpu.VMEM((WIDE, ROWS, LANES), f32),
            pltpu.VMEM((4, WIDE, ROWS, LANES), f32),
            pltpu.VMEM((WIDE, ROWS, LANES), f32),
            pltpu.VMEM((WIDE, 2 * TERMS, LANES), f32),
            pltpu.VMEM((4, WIDE, 2 * TERMS, LANES), f32),
            pltpu.VMEM((4, WIDE, 2 * TERMS, LANES), f32),
            pltpu.VMEM((WIDE, ROWS, LANES), f32),
            pltpu.VMEM((SWEEPS, WIDE, ROWS, LANES), f32),
            pltpu.VMEM((SWEEPS + 1, 2, ROWS, LANES), f32),
            pltpu.VMEM((SWEEPS + 1, 2, ROWS, LANES), f32),
            pltpu.VMEM((SWEEPS + 1, 2, ROWS, LANES), f32),
            pltpu.SemaphoreType.DMA((5,)),
            pltpu.SemaphoreType.DMA((2 * RING,)),
            pltpu.SemaphoreType.DMA((4,)),
            pltpu.SemaphoreType.DMA((4,)),
            pltpu.SemaphoreType.DMA((SWEEPS + 1, 4)),
            pltpu.SemaphoreType.DMA((SWEEPS + 1, 4)),
            pltpu.SemaphoreType.DMA((len(INBOX),)),
            pltpu.SemaphoreType.DMA((len(INBOX),)),
            pltpu.SemaphoreType.DMA((RING + 1,)),
            pltpu.SemaphoreType.DMA((RING + 1,)),
        ],
        compiler_params=pltpu.CompilerParams(
            collective_id=0, has_side_effects=True, vmem_limit_bytes=60 * 1024 * 1024
        ),
        name="galerkin_step",
    )(
        start_field.reshape(modes * wide, lanes),
        right_side.reshape(modes * wide, lanes),
        mean_coef,
        term_coef.reshape(-1, lanes),
        coupling,
        block_mask,
    )
    return (sol.reshape(start_field.shape), res.reshape(start_field.shape))


def solution(mesh):
    placed = (
        P("mode", "sx", "sy"),
        P("mode", "sx", "sy"),
        P("sx", "sy"),
        P(None, "sx", "sy"),
        P(None, None, "mode"),
        P(),
    )
    return jax.shard_map(
        local,
        mesh=mesh,
        in_specs=placed,
        out_specs=(P("mode", "sx", "sy"), P("mode", "sx", "sy")),
        check_vma=False,
    )
```

```python
import functools

import jax
import jax.numpy as jnp
from jax import lax
from jax.experimental import pallas as pl
from jax.experimental.pallas import tpu as pltpu
from jax.sharding import PartitionSpec as P

SWEEPS = 3
REACT = 0.5
THETA = 8.5
DELTA = 8.0
MESH = pl.DeviceIdType.MESH
RING = 8
GROUPS = 2
ROWS = 128
HALF = 64
WIDE = 4
LANES = 128
CELLS = WIDE * LANES
TERMS = 8

QUARTER = 32
UNITS = tuple((p, r, QUARTER, way) for p, r in ((0, 0), (1, 0), (1, HALF)) for r, way in ((r, 1), (r + QUARTER, -1)))

PLAN = (
    ("m", 4), ("y", 4), ("z", 0, 4), ("m", 3), ("y", 3), ("z", 2, 4), ("m", 5), ("y", 5), ("z", 1, 3), ("m", 2),
    ("y", 2), ("z", 3, 3), ("m", 6), ("y", 6), ("m", 1), ("y", 1), ("z", 0, 3), ("m", 7), ("y", 7), ("z", 2, 3),
    ("m", 0), ("z", 4, 4), ("z", 1, 2), ("z", 3, 2), ("z", 0, 2), ("z", 5, 3), ("z", 4, 3), ("z", 1, 1), ("z", 2, 2),
    ("z", 0, 1), ("z", 5, 2), ("z", 4, 2), ("z", 3, 1), ("b",), ("z", 2, 1), ("s",), ("y", 0), ("z", 5, 1), ("z", 4, 1),
)


def hops(unit, way):
    return 4 if UNITS[unit][3] == way else 3


INBOX = {}
for step_ in PLAN:
    if step_[0] == "z":
        INBOX[(1, step_[1], step_[2] - 1)] = len(INBOX)
        INBOX[(-1, step_[1] ^ 1, step_[2] - 1)] = len(INBOX)


def kernel(
    field_in, right_in, mean_in, terms_in, coupling, mask_in, sol, res,
    field, right, mean, terms, mask,
    abuf, lhs_hi, lhs_lo, f_hi, f_lo, part, inbox, ysum, ybox, sbox,
    vp, diffs, base, coef, cbox, dbox, kd, kw, kpack, edge, rowbox, colbox,
    wide, fold, foldbox, corr, direction,
    isem, asem, csend, crecv, hsend, hrecv, rsend, rrecv, ysend, yrecv, wsend, wrecv,
):
    mode = lax.axis_index("mode")
    sx = lax.axis_index("sx")
    sy = lax.axis_index("sy")
    z = lax.rem(mode, RING)
    group = lax.div(mode, RING)
    nx, ny = 4, 4
    zp = (group * RING + lax.rem(z + 1, RING), sx, sy)
    zm = (group * RING + lax.rem(z + RING - 1, RING), sx, sy)
    partner = (lax.rem(mode + RING, 2 * RING), sx, sy)
    xp = (mode, lax.rem(sx + 1, nx), sy)
    xm = (mode, lax.rem(sx + nx - 1, nx), sy)
    yp = (mode, sx, lax.rem(sy + 1, ny))
    ym = (mode, sx, lax.rem(sy + ny - 1, ny))
    corners = ((xp[1], yp[2]), (xm[1], yp[2]), (xp[1], ym[2]), (xm[1], ym[2]))
    corners = tuple((mode, i, j) for i, j in corners)

    barrier = pltpu.get_barrier_semaphore()
    peers = (zp, zm, partner, xp, xm, yp, ym) + corners
    for peer in peers:
        pl.semaphore_signal(barrier, inc=1, device_id=peer, device_id_type=MESH)

    fetch = [
        pltpu.make_async_copy(src, dst, isem.at[i])
        for i, (src, dst) in enumerate(
            ((field_in, field), (mean_in, mean), (terms_in, terms), (mask_in, mask), (right_in, right))
        )
    ]
    for copy in fetch:
        copy.start()

    def block_of(o, p):
        owner = group if p == 1 else 1 - group
        return owner * RING + lax.rem(z + o, RING)

    def load(o, p):
        row = pl.multiple_of(block_of(o, p) * ROWS, ROWS)
        return pltpu.make_async_copy(
            coupling.at[:, pl.ds(row, ROWS), :], abuf.at[o * 2 + p], asem.at[o * 2 + p]
        )

    for o in (4, 3, 5, 2, 6, 1, 0, 7):
        for p in (0, 1):
            load(o, p).start()

    lane = lax.broadcasted_iota(jnp.int32, (ROWS, LANES), 1)

    def edges(planes):
        low, high = None, None
        for x in range(WIDE):
            lo_x = planes[x] if x == 0 else pltpu.roll(planes[x], x, 1)
            hi_x = pltpu.roll(planes[x], x + 1, 1)
            low = lo_x if x == 0 else jnp.where(lane == x, lo_x, low)
            high = hi_x if x == 0 else jnp.where(lane == x, hi_x, high)
        edge[0] = low
        edge[1] = high

    started = []

    def send(src, dst, ssem, rsem, peer):
        copy = pltpu.make_async_remote_copy(
            src_ref=src, dst_ref=dst, send_sem=ssem, recv_sem=rsem, device_id=peer, device_id_type=MESH
        )
        copy.start()
        started.append(copy)
        return copy

    def differences(x):
        center = vp[x]
        up = vp[x - 1] if x > 0 else rowbox[0]
        down = vp[x + 1] if x < WIDE - 1 else rowbox[1]
        lo_col = colbox[0] if x == 0 else pltpu.roll(colbox[0], LANES - x, 1)
        hi_col = pltpu.roll(colbox[1], LANES - 1 - x, 1)
        left = jnp.where(lane == 0, lo_col, pltpu.roll(center, 1, 1))
        after = jnp.where(lane == LANES - 1, hi_col, pltpu.roll(center, LANES - 1, 1))
        return (center - up, center - down, center - left, center - after)

    values = []
    fetch[0].wait()
    for x in range(WIDE):
        plane = field[pl.ds(x, ROWS, stride=WIDE), :]
        vp[x] = plane
        values.append(plane)
    edges(values)
    fetch[1].wait()
    fetch[2].wait()
    for x in range(WIDE):
        coef[x, 0:TERMS, :] = terms[pl.ds(x, TERMS, stride=WIDE), :]
        coef[x, TERMS : 2 * TERMS, :] = jnp.broadcast_to(mean[x : x + 1, :], (TERMS, LANES))

    pl.semaphore_wait(barrier, len(peers))

    coefs = [
        send(coef, cbox.at[0], csend.at[0], crecv.at[0], xp),
        send(coef, cbox.at[1], csend.at[1], crecv.at[1], xm),
        send(coef, cbox.at[2], csend.at[2], crecv.at[2], yp),
        send(coef, cbox.at[3], csend.at[3], crecv.at[3], ym),
    ]
    halo = [
        send(vp.at[WIDE - 1], rowbox.at[0], hsend.at[0], hrecv.at[0], xp),
        send(vp.at[0], rowbox.at[1], hsend.at[1], hrecv.at[1], xm),
        send(edge.at[1], colbox.at[0], hsend.at[2], hrecv.at[2], yp),
        send(edge.at[0], colbox.at[1], hsend.at[3], hrecv.at[3], ym),
    ]
    mean_rows = pl.ds(TERMS, TERMS)
    angles = [
        send(coef.at[:, mean_rows, :], dbox.at[i], csend.at[4 + i], crecv.at[4 + i], corner)
        for i, corner in enumerate(corners)
    ]

    def prepare(o):
        for p in (0, 1):
            load(o, p).wait()
            blk = block_of(o, p)
            for t in range(TERMS):
                value = abuf[o * 2 + p, t] * mask[t, blk, mode].astype(jnp.float32)
                high = value.astype(jnp.bfloat16)
                low = (value - high.astype(jnp.float32)).astype(jnp.bfloat16)
                lhs_hi[o, p * ROWS : (p + 1) * ROWS, t * ROWS : (t + 1) * ROWS] = high
                lhs_lo[o, p * ROWS : (p + 1) * ROWS, t * ROWS : (t + 1) * ROWS] = low

    def multiply(o):
        for n in range(2):
            cols = slice(n * 2 * LANES, (n + 1) * 2 * LANES)
            dot = functools.partial(jnp.dot, preferred_element_type=jnp.float32)
            total = (
                dot(lhs_hi[o], f_hi[:, cols])
                + dot(lhs_hi[o], f_lo[:, cols])
                + dot(lhs_lo[o], f_hi[:, cols])
            )
            part[o, 0, :, cols] = total[0:ROWS]
            part[o, 1, :, cols] = total[ROWS:]

    fetch[3].wait()
    prepare(4)

    for copy in coefs:
        copy.wait_recv()
    thin = lax.broadcasted_iota(jnp.int32, (2 * TERMS, LANES), 1)
    for x in range(WIDE):
        here = coef[x]
        up = coef[x - 1] if x > 0 else cbox[0, WIDE - 1]
        down = coef[x + 1] if x < WIDE - 1 else cbox[1, 0]
        left = jnp.where(thin == 0, pltpu.roll(cbox[2, x], 1, 1), pltpu.roll(here, 1, 1))
        after = jnp.where(thin == LANES - 1, pltpu.roll(cbox[3, x], LANES - 1, 1), pltpu.roll(here, LANES - 1, 1))
        for d, other in enumerate((up, down, left, after)):
            kd[d, x] = 0.5 * (here + other)

    for copy in halo:
        copy.wait_recv()
    for x in range(WIDE):
        for d, delta in enumerate(differences(x)):
            diffs[d, x] = delta

    @pl.loop(0, TERMS)
    def _(t):
        rows = pl.ds(pl.multiple_of(t * ROWS, ROWS), ROWS)
        for x in range(WIDE):
            total = None
            for d in range(4):
                piece = kd[d, x, pl.ds(t, 1), :] * diffs[d, x]
                total = piece if total is None else total + piece
            high = total.astype(jnp.bfloat16)
            cols = slice(x * LANES, (x + 1) * LANES)
            f_hi[rows, cols] = high
            f_lo[rows, cols] = (total - high.astype(jnp.float32)).astype(jnp.bfloat16)

    ring = {}
    crossing = {}
    crossed = set()

    def settle(o):
        if o not in crossed:
            crossed.add(o)
            crossing[o].wait_recv()
            part[o, 1, HALF:, :] += ybox[o]

    def forward(way, unit, o):
        p, first, count, _ = UNITS[unit]
        at = (o * way) % RING
        if unit >= 4:
            settle(at)
        if o < hops(unit, way):
            ring[(way, unit, o)].wait_recv()
            part[at, p, first : first + count, :] += inbox[INBOX[(way, unit, o)]]
        i = INBOX[(way, unit, o - 1)]
        ring[(way, unit, o - 1)] = send(
            part.at[at, p, pl.ds(first, count), :],
            inbox.at[i],
            rsend.at[i],
            rrecv.at[i],
            zp if way == 1 else zm,
        )

    def collect(unit):
        p, first, count, _ = UNITS[unit]
        for way in (1, -1):
            ring[(way, unit, 0)].wait_recv()
        return (
            part[0, p, first : first + count, :]
            + inbox[INBOX[(1, unit, 0)]]
            + inbox[INBOX[(-1, unit, 0)]]
        )

    SPAN = WIDE + 2 * SWEEPS
    DEEP = 2 * SWEEPS

    def layout(rows):
        at = lax.broadcasted_iota(jnp.int32, (rows, LANES), 1)
        plane = lax.shift_right_logical(at * 171, 10)
        return at, plane, at - DEEP * plane

    def gather(planes, plane):
        total = None
        for i, value in planes:
            piece = pltpu.roll(value, DEEP * i + SWEEPS, 1)
            total = piece if total is None else jnp.where(plane == i, piece, total)
        return total

    def join(before, own, after, at, column):
        low = jnp.where(column < SWEEPS, before, own)
        high = jnp.where(column < SWEEPS, own, after)
        return jnp.where(at < 64, low, pltpu.roll(high, 64, 1))

    def pack_shifts(pack):
        return (
            pltpu.roll(pack, DEEP, 1),
            pltpu.roll(pack, LANES - DEEP, 1),
            pltpu.roll(pack, 1, 1),
            pltpu.roll(pack, LANES - 1, 1),
        )

    def side_columns(i, value, pack, at):
        left = jnp.where(at == 0, pltpu.roll(pack, LANES - (DEEP * i + SWEEPS - 1), 1), pltpu.roll(value, 1, 1))
        after = jnp.where(
            at == LANES - 1, pltpu.roll(pack, (60 - DEEP * i) % LANES, 1), pltpu.roll(value, LANES - 1, 1)
        )
        return left, after

    def wide_coefficients():
        for copy in angles:
            copy.wait_recv()
        at, plane, column = layout(TERMS)
        mid = slice(TERMS, 2 * TERMS)

        def column_of(low, own, high):
            rows = [(i, low(i + 1)) for i in range(SWEEPS)]
            rows += [(SWEEPS + x, own(x)) for x in range(WIDE)]
            return rows + [(SWEEPS + WIDE + i, high(i)) for i in range(SWEEPS)]

        here = column_of(lambda x: cbox[0, x, mid], lambda x: coef[x, mid], lambda x: cbox[1, x, mid])
        before = column_of(lambda x: dbox[0, x], lambda x: cbox[2, x, mid], lambda x: dbox[1, x])
        after = column_of(lambda x: dbox[2, x], lambda x: cbox[3, x, mid], lambda x: dbox[3, x])
        pack = join(gather(before, plane), gather(here, plane), gather(after, plane), at, column)
        for d, other in enumerate(pack_shifts(pack)):
            kpack[d] = 0.5 * (pack + other)
        for i in range(1, SPAN - 1):
            value = here[i][1]
            others = (here[i - 1][1], here[i + 1][1]) + side_columns(i, value, pack, at)
            for d, other in enumerate(others):
                kw[d, i] = 0.5 * (value + other)

    FOLD = HALF // 4

    def spread(half):
        rows = pl.ds(half * HALF, HALF)
        at, plane, _ = layout(HALF)
        own = gather([(x, wide[SWEEPS + x, rows, :]) for x in range(WIDE)], plane)
        thin_at = at[0:FOLD]
        total = None
        for g in range(4):
            piece = own[g * FOLD : (g + 1) * FOLD]
            piece = pltpu.roll(piece, 32 * g, 1) if g else piece
            total = piece if total is None else jnp.where(thin_at >= 32 * g, piece, total)
        fold[half] = total
        moves = [
            (wide.at[pl.ds(WIDE, SWEEPS), rows, :], wide.at[pl.ds(0, SWEEPS), rows, :], xp),
            (wide.at[pl.ds(SWEEPS, SWEEPS), rows, :], wide.at[pl.ds(SWEEPS + WIDE, SWEEPS), rows, :], xm),
        ]
        for i, peer in enumerate(corners + (yp, ym)):
            moves.append((fold.at[half], foldbox.at[half, i], peer))
        return [
            send(src, dst, wsend.at[half, i], wrecv.at[half, i], peer) for i, (src, dst, peer) in enumerate(moves)
        ]

    def sweeps(half, moved):
        for copy in moved:
            copy.wait_recv()
        rows = pl.ds(half * HALF, HALF)
        at, plane, column = layout(HALF)

        def unfold(i, shift):
            return jnp.concatenate(
                [pltpu.roll(foldbox[half, i], (shift - 32 * g) % LANES, 1) for g in range(4)], axis=0
            )

        def beside(low, mid, high):
            total = jnp.where(plane < SWEEPS, unfold(low, -DEEP), unfold(mid, DEEP * SWEEPS))
            return jnp.where(plane >= SWEEPS + WIDE, unfold(high, DEEP * (SWEEPS + WIDE)), total)

        here = [(i, wide[i, rows, :]) for i in range(SPAN)]
        pack = join(beside(0, 4, 1), gather(here, plane), beside(2, 5, 3), at, column)
        wide[SPAN, rows, :] = pack
        for i in range(SPAN + 1):
            value = wide[i, rows, :] * (1.0 / THETA)
            corr[0, i, rows, :] = value
            direction[i, rows, :] = value

        sigma = THETA / DELTA
        rho = 1.0 / sigma
        for sweep in range(SWEEPS):
            now, later = sweep % 2, (sweep + 1) % 2
            rho_next = 1.0 / (2.0 * sigma - rho)
            pack = corr[now, SPAN, rows, :]

            def advance(i, value, others, coefficients):
                applied = REACT * value
                for d in range(4):
                    applied = applied + coefficients(d) * (value - others[d])
                step = rho_next * rho * direction[i, rows, :]
                step = step + (2.0 * rho_next / DELTA) * (wide[i, rows, :] - applied)
                return step

            for i in range(sweep + 1, SPAN - 1 - sweep):
                value = corr[now, i, rows, :]
                others = (corr[now, i - 1, rows, :], corr[now, i + 1, rows, :]) + side_columns(i, value, pack, at)
                step = advance(i, value, others, lambda d: kw[d, i, 0:1, :])
                if sweep < SWEEPS - 1:
                    direction[i, rows, :] = step
                    corr[later, i, rows, :] = value + step
                else:
                    x = i - SWEEPS
                    sol[pl.ds(half * HALF * WIDE + x, HALF, stride=WIDE), :] = vp[x, rows, :] + (value + step)
            if sweep < SWEEPS - 1:
                step = advance(SPAN, pack, pack_shifts(pack), lambda d: kpack[d, 0:1, :])
                direction[SPAN, rows, :] = step
                corr[later, SPAN, rows, :] = pack + step
            rho = rho_next

    sums = None
    for step in PLAN:
        if step[0] == "m":
            if step[1] != 4:
                prepare(step[1])
            multiply(step[1])
        elif step[0] == "z":
            forward(1, step[1], step[2])
            forward(-1, step[1] ^ 1, step[2])
        elif step[0] == "y":
            o = step[1]
            crossing[o] = send(
                part.at[o, 0, pl.ds(HALF, HALF), :], ybox.at[o], ysend.at[o], yrecv.at[o], partner
            )
        elif step[0] == "s":
            for unit in (0, 1):
                ysum[unit * QUARTER : (unit + 1) * QUARTER] = collect(unit)
            sums = send(ysum, sbox, ysend.at[RING], yrecv.at[RING], partner)
        else:
            fetch[4].wait()
            for x in range(WIDE):
                total = REACT * vp[x]
                for d in range(4):
                    total = total + kd[d, x, TERMS : TERMS + 1, :] * diffs[d, x]
                base[x] = right[pl.ds(x, ROWS, stride=WIDE), :] - total
            wide_coefficients()

    def finish(unit, extra):
        first = UNITS[unit][1]
        rows = slice(first, first + QUARTER)
        total = collect(unit)
        if extra is not None:
            total = total + extra
        for x in range(WIDE):
            value = base[x, rows, :] - total[:, x * LANES : (x + 1) * LANES]
            wide[SWEEPS + x, rows, :] = value
            res[pl.ds(first * WIDE + x, QUARTER, stride=WIDE), :] = value

    sums.wait_recv()
    finish(2, sbox[0:QUARTER])
    finish(3, sbox[QUARTER:HALF])
    early = spread(0)
    settle(0)
    finish(4, None)
    finish(5, None)
    late = spread(1)
    sweeps(0, early)
    sweeps(1, late)

    for copy in started:
        copy.wait_send()


def local(start_field, right_side, mean_coef, term_coef, coupling, block_mask):
    modes, wide, lanes = start_field.shape
    f32, bf16 = jnp.float32, jnp.bfloat16
    vmem = pl.BlockSpec(memory_space=pltpu.VMEM)
    flat = jax.ShapeDtypeStruct((modes * wide, lanes), f32)
    sol, res = pl.pallas_call(
        kernel,
        out_shape=(flat, flat),
        in_specs=[pl.BlockSpec(memory_space=pltpu.HBM)] * 6,
        out_specs=(vmem, vmem),
        scratch_shapes=[
            pltpu.VMEM((modes * wide, lanes), f32),
            pltpu.VMEM((modes * wide, lanes), f32),
            pltpu.VMEM(mean_coef.shape, f32),
            pltpu.VMEM((TERMS * WIDE, lanes), f32),
            pltpu.SMEM(block_mask.shape, jnp.int32),
            pltpu.VMEM((2 * RING, TERMS, ROWS, ROWS), f32),
            pltpu.VMEM((RING, 2 * ROWS, TERMS * ROWS), bf16),
            pltpu.VMEM((RING, 2 * ROWS, TERMS * ROWS), bf16),
            pltpu.VMEM((TERMS * ROWS, CELLS), bf16),
            pltpu.VMEM((TERMS * ROWS, CELLS), bf16),
            pltpu.VMEM((RING, 2, ROWS, CELLS), f32),
            pltpu.VMEM((len(INBOX), QUARTER, CELLS), f32),
            pltpu.VMEM((HALF, CELLS), f32),
            pltpu.VMEM((RING, HALF, CELLS), f32),
            pltpu.VMEM((HALF, CELLS), f32),
            pltpu.VMEM((WIDE, ROWS, LANES), f32),
            pltpu.VMEM((4, WIDE, ROWS, LANES), f32),
            pltpu.VMEM((WIDE, ROWS, LANES), f32),
            pltpu.VMEM((WIDE, 2 * TERMS, LANES), f32),
            pltpu.VMEM((4, WIDE, 2 * TERMS, LANES), f32),
            pltpu.VMEM((4, WIDE, TERMS, LANES), f32),
            pltpu.VMEM((4, WIDE, 2 * TERMS, LANES), f32),
            pltpu.VMEM((4, WIDE + 2 * SWEEPS, TERMS, LANES), f32),
            pltpu.VMEM((4, TERMS, LANES), f32),
            pltpu.VMEM((2, ROWS, LANES), f32),
            pltpu.VMEM((2, ROWS, LANES), f32),
            pltpu.VMEM((2, ROWS, LANES), f32),
            pltpu.VMEM((WIDE + 2 * SWEEPS + 1, ROWS, LANES), f32),
            pltpu.VMEM((2, HALF // 4, LANES), f32),
            pltpu.VMEM((2, 6, HALF // 4, LANES), f32),
            pltpu.VMEM((2, WIDE + 2 * SWEEPS + 1, ROWS, LANES), f32),
            pltpu.VMEM((WIDE + 2 * SWEEPS + 1, ROWS, LANES), f32),
            pltpu.SemaphoreType.DMA((5,)),
            pltpu.SemaphoreType.DMA((2 * RING,)),
            pltpu.SemaphoreType.DMA((8,)),
            pltpu.SemaphoreType.DMA((8,)),
            pltpu.SemaphoreType.DMA((4,)),
            pltpu.SemaphoreType.DMA((4,)),
            pltpu.SemaphoreType.DMA((len(INBOX),)),
            pltpu.SemaphoreType.DMA((len(INBOX),)),
            pltpu.SemaphoreType.DMA((RING + 1,)),
            pltpu.SemaphoreType.DMA((RING + 1,)),
            pltpu.SemaphoreType.DMA((2, 8)),
            pltpu.SemaphoreType.DMA((2, 8)),
        ],
        compiler_params=pltpu.CompilerParams(
            collective_id=0, has_side_effects=True, vmem_limit_bytes=48000 * 1024
        ),
        name="galerkin_step",
    )(
        *(
            pltpu.with_memory_space_constraint(value, pltpu.HBM)
            for value in (
                start_field.reshape(modes * wide, lanes),
                right_side.reshape(modes * wide, lanes),
                mean_coef,
                term_coef.reshape(-1, lanes),
                coupling,
                block_mask,
            )
        )
    )
    return (sol.reshape(start_field.shape), res.reshape(start_field.shape))


def solution(mesh):
    placed = (
        P("mode", "sx", "sy"),
        P("mode", "sx", "sy"),
        P("sx", "sy"),
        P(None, "sx", "sy"),
        P(None, None, "mode"),
        P(),
    )
    return jax.shard_map(
        local,
        mesh=mesh,
        in_specs=placed,
        out_specs=(P("mode", "sx", "sy"), P("mode", "sx", "sy")),
        check_vma=False,
    )
```

```python
import functools

import jax
import jax.numpy as jnp
from jax import lax
from jax.experimental import pallas as pl
from jax.experimental.pallas import tpu as pltpu
from jax.sharding import PartitionSpec as P

SWEEPS = 3
REACT = 0.5
THETA = 8.5
DELTA = 8.0
MESH = pl.DeviceIdType.MESH
RING = 8
GROUPS = 2
ROWS = 128
HALF = 64
WIDE = 4
LANES = 128
CELLS = WIDE * LANES
TERMS = 8

QUARTER = 32
UNITS = tuple((p, r, QUARTER, way) for p, r in ((0, 0), (1, 0), (1, HALF)) for r, way in ((r, 1), (r + QUARTER, -1)))

PLAN = (
    ("m", 4, 0), ("y", 4), ("z", 1, 0, 4), ("z", -1, 1, 4), ("m", 4, 1), ("z", 1, 2, 4), ("z", -1, 3, 4),
    ("m", 3, 2), ("y", 3), ("z", 1, 3, 3), ("m", 5, 2), ("y", 5), ("z", -1, 0, 3), ("z", 1, 1, 3), ("z", -1, 2, 3),
    ("m", 2, 2), ("y", 2), ("m", 6, 2), ("y", 6), ("z", 1, 0, 3), ("z", -1, 1, 3), ("m", 1, 2), ("y", 1),
    ("z", 1, 4, 4), ("z", -1, 5, 4), ("m", 7, 2), ("y", 7), ("z", 1, 2, 3), ("z", -1, 3, 3), ("m", 0, 2),
    ("z", -1, 0, 2), ("z", 1, 3, 2), ("b",), ("z", 1, 1, 2), ("z", -1, 2, 2), ("z", 1, 0, 2), ("z", -1, 1, 2),
    ("z", 1, 4, 3), ("z", -1, 4, 3), ("z", 1, 5, 3), ("z", -1, 5, 3), ("z", 1, 2, 2), ("z", -1, 0, 1),
    ("z", 1, 1, 1), ("z", -1, 3, 2), ("z", 1, 0, 1), ("z", -1, 1, 1), ("y", 0), ("z", 1, 4, 2), ("z", -1, 4, 2),
    ("z", 1, 5, 2), ("z", -1, 5, 2), ("z", 1, 2, 1), ("z", -1, 2, 1), ("z", 1, 3, 1), ("z", -1, 3, 1), ("s", 0),
    ("s", 1), ("z", 1, 4, 1), ("z", -1, 4, 1), ("z", 1, 5, 1), ("z", -1, 5, 1), ("f", 0), ("f", 1), ("f", 2),
    ("f", 3), ("c", 0), ("c", 1), ("c", 2), ("c", 3),
)


def hops(unit, way):
    return 4 if UNITS[unit][3] == way else 3


INBOX = {}
for step_ in PLAN:
    if step_[0] == "z":
        INBOX[(step_[1], step_[2], step_[3] - 1)] = len(INBOX)


def kernel(
    field_in, right_in, mean_in, terms_in, coupling, mask_in, sol, res,
    field, right, mean, terms, mask,
    abuf, lhs_hi, lhs_lo, f_hi, f_lo, part, inbox, ysum, ybox, sbox,
    vp, diffs, base, coef, mrow, cxbox, cybox, mbox, kd, kw, kpack, edge, rowbox, colbox,
    wide, fold, foldbox, corr, direction,
    isem, asem, csend, crecv, msend, mrecv, hsend, hrecv, rsend, rrecv, ysend, yrecv, wsend, wrecv,
):
    mode = lax.axis_index("mode")
    sx = lax.axis_index("sx")
    sy = lax.axis_index("sy")
    z = lax.rem(mode, RING)
    group = lax.div(mode, RING)
    nx, ny = 4, 4
    zp = (group * RING + lax.rem(z + 1, RING), sx, sy)
    zm = (group * RING + lax.rem(z + RING - 1, RING), sx, sy)
    partner = (lax.rem(mode + RING, 2 * RING), sx, sy)
    xp = (mode, lax.rem(sx + 1, nx), sy)
    xm = (mode, lax.rem(sx + nx - 1, nx), sy)
    yp = (mode, sx, lax.rem(sy + 1, ny))
    ym = (mode, sx, lax.rem(sy + ny - 1, ny))
    corners = ((xp[1], yp[2]), (xm[1], yp[2]), (xp[1], ym[2]), (xm[1], ym[2]))
    corners = tuple((mode, i, j) for i, j in corners)

    barrier = pltpu.get_barrier_semaphore()
    peers = (zp, zm, partner, xp, xm, yp, ym) + corners
    for peer in peers:
        pl.semaphore_signal(barrier, inc=1, device_id=peer, device_id_type=MESH)

    fetch = [
        pltpu.make_async_copy(src, dst, isem.at[i])
        for i, (src, dst) in enumerate(
            ((field_in, field), (mean_in, mean), (terms_in, terms), (mask_in, mask), (right_in, right))
        )
    ]
    for copy in fetch:
        copy.start()

    def block_of(o, p):
        owner = group if p == 1 else 1 - group
        return owner * RING + lax.rem(z + o, RING)

    def load(o, p):
        row = pl.multiple_of(block_of(o, p) * ROWS, ROWS)
        return pltpu.make_async_copy(
            coupling.at[:, pl.ds(row, ROWS), :], abuf.at[o * 2 + p], asem.at[o * 2 + p]
        )

    for o in (4, 3, 5, 2, 6, 1, 0, 7):
        for p in (0, 1):
            load(o, p).start()

    lane = lax.broadcasted_iota(jnp.int32, (ROWS, LANES), 1)

    def edges(planes):
        low, high = None, None
        for x in range(WIDE):
            lo_x = planes[x] if x == 0 else pltpu.roll(planes[x], x, 1)
            hi_x = pltpu.roll(planes[x], x + 1, 1)
            low = lo_x if x == 0 else jnp.where(lane == x, lo_x, low)
            high = hi_x if x == 0 else jnp.where(lane == x, hi_x, high)
        edge[0] = low
        edge[1] = high

    started = []

    def send(src, dst, ssem, rsem, peer):
        copy = pltpu.make_async_remote_copy(
            src_ref=src, dst_ref=dst, send_sem=ssem, recv_sem=rsem, device_id=peer, device_id_type=MESH
        )
        copy.start()
        started.append(copy)
        return copy

    def differences(x):
        center = vp[x]
        up = vp[x - 1] if x > 0 else rowbox[0]
        down = vp[x + 1] if x < WIDE - 1 else rowbox[1]
        lo_col = colbox[0] if x == 0 else pltpu.roll(colbox[0], LANES - x, 1)
        hi_col = pltpu.roll(colbox[1], LANES - 1 - x, 1)
        left = jnp.where(lane == 0, lo_col, pltpu.roll(center, 1, 1))
        after = jnp.where(lane == LANES - 1, hi_col, pltpu.roll(center, LANES - 1, 1))
        return (center - up, center - down, center - left, center - after)

    values = []
    fetch[0].wait()
    for x in range(WIDE):
        plane = field[pl.ds(x, ROWS, stride=WIDE), :]
        vp[x] = plane
        values.append(plane)
    edges(values)
    fetch[1].wait()
    fetch[2].wait()
    for x in range(WIDE):
        coef[x] = terms[pl.ds(x, TERMS, stride=WIDE), :]
    mrow[0:WIDE] = mean[...]
    mrow[WIDE:] = mean[...]

    pl.semaphore_wait(barrier, len(peers))

    coefs = [
        send(coef.at[WIDE - 1], cxbox.at[0], csend.at[0], crecv.at[0], xp),
        send(coef.at[0], cxbox.at[1], csend.at[1], crecv.at[1], xm),
        send(coef, cybox.at[0], csend.at[2], crecv.at[2], yp),
        send(coef, cybox.at[1], csend.at[3], crecv.at[3], ym),
    ]
    means = [
        send(mrow, mbox.at[i], msend.at[i], mrecv.at[i], peer) for i, peer in enumerate((xp, xm, yp, ym))
    ]
    halo = [
        send(vp.at[WIDE - 1], rowbox.at[0], hsend.at[0], hrecv.at[0], xp),
        send(vp.at[0], rowbox.at[1], hsend.at[1], hrecv.at[1], xm),
        send(edge.at[1], colbox.at[0], hsend.at[2], hrecv.at[2], yp),
        send(edge.at[0], colbox.at[1], hsend.at[3], hrecv.at[3], ym),
    ]
    angles = [
        send(mrow, mbox.at[4 + i], msend.at[4 + i], mrecv.at[4 + i], corner) for i, corner in enumerate(corners)
    ]

    def prepare(o):
        for p in (0, 1):
            load(o, p).wait()
            blk = block_of(o, p)
            for t in range(TERMS):
                value = abuf[o * 2 + p, t] * mask[t, blk, mode].astype(jnp.float32)
                high = value.astype(jnp.bfloat16)
                low = (value - high.astype(jnp.float32)).astype(jnp.bfloat16)
                lhs_hi[o, p * ROWS : (p + 1) * ROWS, t * ROWS : (t + 1) * ROWS] = high
                lhs_lo[o, p * ROWS : (p + 1) * ROWS, t * ROWS : (t + 1) * ROWS] = low

    def multiply(o, parts):
        first, last = parts[0] * ROWS, (parts[-1] + 1) * ROWS
        for n in range(2):
            cols = slice(n * 2 * LANES, (n + 1) * 2 * LANES)
            dot = functools.partial(jnp.dot, preferred_element_type=jnp.float32)
            total = (
                dot(lhs_hi[o, first:last], f_hi[:, cols])
                + dot(lhs_hi[o, first:last], f_lo[:, cols])
                + dot(lhs_lo[o, first:last], f_hi[:, cols])
            )
            for i, p in enumerate(parts):
                part[o, p, :, cols] = total[i * ROWS : (i + 1) * ROWS]

    fetch[3].wait()
    prepare(4)

    for copy in coefs + means:
        copy.wait_recv()

    def mean_plane(box, x):
        return jnp.broadcast_to(box[x : x + 1, :], (TERMS, LANES))

    thin = lax.broadcasted_iota(jnp.int32, (TERMS, LANES), 1)

    def coefficients(x, rows, own, low, high, before, after):
        up = own(x - 1) if x > 0 else low
        down = own(x + 1) if x < WIDE - 1 else high
        here = own(x)
        left = jnp.where(thin == 0, pltpu.roll(before(x), 1, 1), pltpu.roll(here, 1, 1))
        right_of = jnp.where(thin == LANES - 1, pltpu.roll(after(x), LANES - 1, 1), pltpu.roll(here, LANES - 1, 1))
        for d, other in enumerate((up, down, left, right_of)):
            kd[d, x, rows, :] = 0.5 * (here + other)

    for x in range(WIDE):
        coefficients(
            x, slice(0, TERMS), lambda i: coef[i], cxbox[0], cxbox[1], lambda i: cybox[0, i], lambda i: cybox[1, i]
        )
        coefficients(
            x,
            slice(TERMS, 2 * TERMS),
            lambda i: mean_plane(mrow, i),
            mean_plane(mbox.at[0], WIDE - 1),
            mean_plane(mbox.at[1], 0),
            lambda i: mean_plane(mbox.at[2], i),
            lambda i: mean_plane(mbox.at[3], i),
        )

    for copies, planes in ((halo[2:], (1, 2)), (halo[:2], (0, 3))):
        for copy in copies:
            copy.wait_recv()
        for x in planes:
            for d, delta in enumerate(differences(x)):
                diffs[d, x] = delta

        @pl.loop(0, TERMS)
        def _(t, planes=planes):
            rows = pl.ds(pl.multiple_of(t * ROWS, ROWS), ROWS)
            for x in planes:
                total = None
                for d in range(4):
                    piece = kd[d, x, pl.ds(t, 1), :] * diffs[d, x]
                    total = piece if total is None else total + piece
                high = total.astype(jnp.bfloat16)
                cols = slice(x * LANES, (x + 1) * LANES)
                f_hi[rows, cols] = high
                f_lo[rows, cols] = (total - high.astype(jnp.float32)).astype(jnp.bfloat16)

    ring = {}
    crossing = {}
    crossed = set()

    def settle(o):
        if o not in crossed:
            crossed.add(o)
            crossing[o].wait_recv()
            part[o, 1, HALF:, :] += ybox[o]

    def forward(way, unit, o):
        p, first, count, _ = UNITS[unit]
        at = (o * way) % RING
        if unit >= 4:
            settle(at)
        if o < hops(unit, way):
            ring[(way, unit, o)].wait_recv()
            part[at, p, first : first + count, :] += inbox[INBOX[(way, unit, o)]]
        i = INBOX[(way, unit, o - 1)]
        ring[(way, unit, o - 1)] = send(
            part.at[at, p, pl.ds(first, count), :],
            inbox.at[i],
            rsend.at[i],
            rrecv.at[i],
            zp if way == 1 else zm,
        )

    def collect(unit):
        p, first, count, _ = UNITS[unit]
        for way in (1, -1):
            ring[(way, unit, 0)].wait_recv()
        return (
            part[0, p, first : first + count, :]
            + inbox[INBOX[(1, unit, 0)]]
            + inbox[INBOX[(-1, unit, 0)]]
        )

    SPAN = WIDE + 2 * SWEEPS
    DEEP = 2 * SWEEPS

    def layout(rows):
        at = lax.broadcasted_iota(jnp.int32, (rows, LANES), 1)
        plane = lax.shift_right_logical(at * 171, 10)
        return at, plane, at - DEEP * plane

    def gather(planes, plane):
        total = None
        for i, value in planes:
            piece = pltpu.roll(value, DEEP * i + SWEEPS, 1)
            total = piece if total is None else jnp.where(plane == i, piece, total)
        return total

    def join(before, own, after, at, column):
        low = jnp.where(column < SWEEPS, before, own)
        high = jnp.where(column < SWEEPS, own, after)
        return jnp.where(at < 64, low, pltpu.roll(high, 64, 1))

    def pack_shifts(pack):
        return (
            pltpu.roll(pack, DEEP, 1),
            pltpu.roll(pack, LANES - DEEP, 1),
            pltpu.roll(pack, 1, 1),
            pltpu.roll(pack, LANES - 1, 1),
        )

    def side_columns(i, value, pack, at):
        left = jnp.where(at == 0, pltpu.roll(pack, LANES - (DEEP * i + SWEEPS - 1), 1), pltpu.roll(value, 1, 1))
        after = jnp.where(
            at == LANES - 1, pltpu.roll(pack, (60 - DEEP * i) % LANES, 1), pltpu.roll(value, LANES - 1, 1)
        )
        return left, after

    def wide_coefficients():
        for copy in angles:
            copy.wait_recv()
        at, plane, column = layout(TERMS)

        def column_of(low, own, high):
            rows = [(i, low(i + 1)) for i in range(SWEEPS)]
            rows += [(SWEEPS + x, own(x)) for x in range(WIDE)]
            return rows + [(SWEEPS + WIDE + i, high(i)) for i in range(SWEEPS)]

        boxes = [mbox.at[i] for i in range(8)]
        here, before, after = (
            column_of(*(functools.partial(mean_plane, box) for box in group))
            for group in (
                (boxes[0], mrow, boxes[1]),
                (boxes[4], boxes[2], boxes[5]),
                (boxes[6], boxes[3], boxes[7]),
            )
        )
        pack = join(gather(before, plane), gather(here, plane), gather(after, plane), at, column)
        for d, other in enumerate(pack_shifts(pack)):
            kpack[d] = 0.5 * (pack + other)
        for i in range(1, SPAN - 1):
            value = here[i][1]
            others = (here[i - 1][1], here[i + 1][1]) + side_columns(i, value, pack, at)
            for d, other in enumerate(others):
                kw[d, i] = 0.5 * (value + other)

    FOLD = QUARTER // 4

    def spread(part_of):
        rows = pl.ds(part_of * QUARTER, QUARTER)
        at, plane, _ = layout(QUARTER)
        own = gather([(x, wide[SWEEPS + x, rows, :]) for x in range(WIDE)], plane)
        thin_at = at[0:FOLD]
        total = None
        for g in range(4):
            piece = own[g * FOLD : (g + 1) * FOLD]
            piece = pltpu.roll(piece, 32 * g, 1) if g else piece
            total = piece if total is None else jnp.where(thin_at >= 32 * g, piece, total)
        fold[part_of] = total
        moves = [(fold.at[part_of], foldbox.at[part_of, i], peer) for i, peer in enumerate(corners + (yp, ym))]
        moves += [
            (wide.at[pl.ds(WIDE, SWEEPS), rows, :], wide.at[pl.ds(0, SWEEPS), rows, :], xp),
            (wide.at[pl.ds(SWEEPS, SWEEPS), rows, :], wide.at[pl.ds(SWEEPS + WIDE, SWEEPS), rows, :], xm),
        ]
        return [
            send(src, dst, wsend.at[part_of, i], wrecv.at[part_of, i], peer)
            for i, (src, dst, peer) in enumerate(moves)
        ]

    def sweeps(part_of, moved):
        for copy in moved:
            copy.wait_recv()
        rows = pl.ds(part_of * QUARTER, QUARTER)
        at, plane, column = layout(QUARTER)

        def unfold(i, shift):
            return jnp.concatenate(
                [pltpu.roll(foldbox[part_of, i], (shift - 32 * g) % LANES, 1) for g in range(4)], axis=0
            )

        def beside(low, mid, high):
            total = jnp.where(plane < SWEEPS, unfold(low, -DEEP), unfold(mid, DEEP * SWEEPS))
            return jnp.where(plane >= SWEEPS + WIDE, unfold(high, DEEP * (SWEEPS + WIDE)), total)

        here = [(i, wide[i, rows, :]) for i in range(SPAN)]
        pack = join(beside(0, 4, 1), gather(here, plane), beside(2, 5, 3), at, column)
        wide[SPAN, rows, :] = pack
        for i in range(SPAN + 1):
            value = wide[i, rows, :] * (1.0 / THETA)
            corr[0, i, rows, :] = value
            direction[i, rows, :] = value

        sigma = THETA / DELTA
        rho = 1.0 / sigma
        for sweep in range(SWEEPS):
            now, later = sweep % 2, (sweep + 1) % 2
            rho_next = 1.0 / (2.0 * sigma - rho)
            pack = corr[now, SPAN, rows, :]

            def advance(i, value, others, coefficients):
                applied = REACT * value
                for d in range(4):
                    applied = applied + coefficients(d) * (value - others[d])
                step = rho_next * rho * direction[i, rows, :]
                step = step + (2.0 * rho_next / DELTA) * (wide[i, rows, :] - applied)
                return step

            for i in range(sweep + 1, SPAN - 1 - sweep):
                value = corr[now, i, rows, :]
                others = (corr[now, i - 1, rows, :], corr[now, i + 1, rows, :]) + side_columns(i, value, pack, at)
                step = advance(i, value, others, lambda d: kw[d, i, 0:1, :])
                if sweep < SWEEPS - 1:
                    direction[i, rows, :] = step
                    corr[later, i, rows, :] = value + step
                else:
                    x = i - SWEEPS
                    sol[pl.ds(part_of * QUARTER * WIDE + x, QUARTER, stride=WIDE), :] = vp[x, rows, :] + (value + step)
            if sweep < SWEEPS - 1:
                step = advance(SPAN, pack, pack_shifts(pack), lambda d: kpack[d, 0:1, :])
                direction[SPAN, rows, :] = step
                corr[later, SPAN, rows, :] = pack + step
            rho = rho_next

    def prepare_residual():
        fetch[4].wait()
        for x in range(WIDE):
            total = REACT * vp[x]
            for d in range(4):
                total = total + kd[d, x, TERMS : TERMS + 1, :] * diffs[d, x]
            base[x] = right[pl.ds(x, ROWS, stride=WIDE), :] - total
        wide_coefficients()

    sums = {}

    def finish(quarter):
        first = quarter * QUARTER
        rows = slice(first, first + QUARTER)
        if quarter in sums:
            sums[quarter].wait_recv()
            total = collect(2 + quarter) + sbox[rows]
        else:
            settle(0)
            total = collect(2 + quarter)
        for x in range(WIDE):
            value = base[x, rows, :] - total[:, x * LANES : (x + 1) * LANES]
            wide[SWEEPS + x, rows, :] = value
            res[pl.ds(first * WIDE + x, QUARTER, stride=WIDE), :] = value
        return spread(quarter)

    spreads = {}
    for step in PLAN:
        what = step[0]
        if what == "m":
            if step[1] != 4:
                prepare(step[1])
            multiply(step[1], ((0,), (1,), (0, 1))[step[2]])
        elif what == "z":
            forward(*step[1:])
        elif what == "y":
            o = step[1]
            crossing[o] = send(
                part.at[o, 0, pl.ds(HALF, HALF), :], ybox.at[o], ysend.at[o], yrecv.at[o], partner
            )
        elif what == "s":
            i = step[1]
            rows = pl.ds(i * QUARTER, QUARTER)
            ysum[rows, :] = collect(i)
            sums[i] = send(ysum.at[rows], sbox.at[rows], ysend.at[RING + i], yrecv.at[RING + i], partner)
        elif what == "b":
            prepare_residual()
        elif what == "f":
            spreads[step[1]] = finish(step[1])
        else:
            sweeps(step[1], spreads[step[1]])

    for copy in started:
        copy.wait_send()


def place(sol, res, sol_out, res_out, sem):
    copies = [pltpu.make_async_copy(sol, sol_out, sem.at[0]), pltpu.make_async_copy(res, res_out, sem.at[1])]
    for copy in copies:
        copy.start()
    for copy in copies:
        copy.wait()


def local(start_field, right_side, mean_coef, term_coef, coupling, block_mask):
    modes, wide, lanes = start_field.shape
    f32, bf16 = jnp.float32, jnp.bfloat16
    vmem = pl.BlockSpec(memory_space=pltpu.VMEM)
    flat = jax.ShapeDtypeStruct((modes * wide, lanes), f32)
    sol, res = pl.pallas_call(
        kernel,
        out_shape=(flat, flat),
        in_specs=[pl.BlockSpec(memory_space=pltpu.HBM)] * 6,
        out_specs=(vmem, vmem),
        scratch_shapes=[
            pltpu.VMEM((modes * wide, lanes), f32),
            pltpu.VMEM((modes * wide, lanes), f32),
            pltpu.VMEM(mean_coef.shape, f32),
            pltpu.VMEM((TERMS * WIDE, lanes), f32),
            pltpu.SMEM(block_mask.shape, jnp.int32),
            pltpu.VMEM((2 * RING, TERMS, ROWS, ROWS), f32),
            pltpu.VMEM((RING, 2 * ROWS, TERMS * ROWS), bf16),
            pltpu.VMEM((RING, 2 * ROWS, TERMS * ROWS), bf16),
            pltpu.VMEM((TERMS * ROWS, CELLS), bf16),
            pltpu.VMEM((TERMS * ROWS, CELLS), bf16),
            pltpu.VMEM((RING, 2, ROWS, CELLS), f32),
            pltpu.VMEM((len(INBOX), QUARTER, CELLS), f32),
            pltpu.VMEM((HALF, CELLS), f32),
            pltpu.VMEM((RING, HALF, CELLS), f32),
            pltpu.VMEM((HALF, CELLS), f32),
            pltpu.VMEM((WIDE, ROWS, LANES), f32),
            pltpu.VMEM((4, WIDE, ROWS, LANES), f32),
            pltpu.VMEM((WIDE, ROWS, LANES), f32),
            pltpu.VMEM((WIDE, TERMS, LANES), f32),
            pltpu.VMEM((TERMS, LANES), f32),
            pltpu.VMEM((2, TERMS, LANES), f32),
            pltpu.VMEM((2, WIDE, TERMS, LANES), f32),
            pltpu.VMEM((8, TERMS, LANES), f32),
            pltpu.VMEM((4, WIDE, 2 * TERMS, LANES), f32),
            pltpu.VMEM((4, WIDE + 2 * SWEEPS, TERMS, LANES), f32),
            pltpu.VMEM((4, TERMS, LANES), f32),
            pltpu.VMEM((2, ROWS, LANES), f32),
            pltpu.VMEM((2, ROWS, LANES), f32),
            pltpu.VMEM((2, ROWS, LANES), f32),
            pltpu.VMEM((WIDE + 2 * SWEEPS + 1, ROWS, LANES), f32),
            pltpu.VMEM((4, QUARTER // 4, LANES), f32),
            pltpu.VMEM((4, 6, QUARTER // 4, LANES), f32),
            pltpu.VMEM((2, WIDE + 2 * SWEEPS + 1, ROWS, LANES), f32),
            pltpu.VMEM((WIDE + 2 * SWEEPS + 1, ROWS, LANES), f32),
            pltpu.SemaphoreType.DMA((5,)),
            pltpu.SemaphoreType.DMA((2 * RING,)),
            pltpu.SemaphoreType.DMA((4,)),
            pltpu.SemaphoreType.DMA((4,)),
            pltpu.SemaphoreType.DMA((8,)),
            pltpu.SemaphoreType.DMA((8,)),
            pltpu.SemaphoreType.DMA((4,)),
            pltpu.SemaphoreType.DMA((4,)),
            pltpu.SemaphoreType.DMA((len(INBOX),)),
            pltpu.SemaphoreType.DMA((len(INBOX),)),
            pltpu.SemaphoreType.DMA((RING + 2,)),
            pltpu.SemaphoreType.DMA((RING + 2,)),
            pltpu.SemaphoreType.DMA((4, 8)),
            pltpu.SemaphoreType.DMA((4, 8)),
        ],
        compiler_params=pltpu.CompilerParams(
            collective_id=0, has_side_effects=True, vmem_limit_bytes=48000 * 1024
        ),
        name="galerkin_step",
    )(
        *(
            pltpu.with_memory_space_constraint(value, pltpu.HBM)
            for value in (
                start_field.reshape(modes * wide, lanes),
                right_side.reshape(modes * wide, lanes),
                mean_coef,
                term_coef.reshape(-1, lanes),
                coupling,
                block_mask,
            )
        )
    )
    hbm = pl.BlockSpec(memory_space=pltpu.HBM)
    sol, res = pl.pallas_call(
        place,
        out_shape=(flat, flat),
        in_specs=[vmem, vmem],
        out_specs=(hbm, hbm),
        scratch_shapes=[pltpu.SemaphoreType.DMA((2,))],
        compiler_params=pltpu.CompilerParams(vmem_limit_bytes=1 << 20),
        name="place",
    )(sol, res)
    return (sol.reshape(start_field.shape), res.reshape(start_field.shape))


def solution(mesh):
    placed = (
        P("mode", "sx", "sy"),
        P("mode", "sx", "sy"),
        P("sx", "sy"),
        P(None, "sx", "sy"),
        P(None, None, "mode"),
        P(),
    )
    return jax.shard_map(
        local,
        mesh=mesh,
        in_specs=placed,
        out_specs=(P("mode", "sx", "sy"), P("mode", "sx", "sy")),
        check_vma=False,
    )
```

```python
import functools

import jax
import jax.numpy as jnp
from jax import lax
from jax.experimental import pallas as pl
from jax.experimental.pallas import tpu as pltpu
from jax.sharding import PartitionSpec as P

SWEEPS = 3
REACT = 0.5
THETA = 8.5
DELTA = 8.0
MESH = pl.DeviceIdType.MESH
RING = 8
GROUPS = 2
ROWS = 128
WIDE = 4
LANES = 128
CELLS = WIDE * LANES
TERMS = 8

EARLY = (32, 24)
LATE = (32, 40)
CROSSING = sum(EARLY)
UNITS = tuple(
    (p, first + (rows[0] if way < 0 else 0), rows[way < 0], way)
    for p, first, rows in ((0, 0, EARLY), (1, 0, EARLY), (1, CROSSING, LATE))
    for way in (1, -1)
)
MOST = max(EARLY + LATE)
GROUP = WIDE * 2 * SWEEPS

PLAN = (
    ("m", 4, 0, 0), ("z", 1, 0, 4, 0), ("z", -1, 1, 4, 0), ("y", 4, 0), ("m", 4, 1, 0), ("z", 1, 2, 4, 0),
    ("z", -1, 3, 4, 0), ("x",), ("m", 4, 2, 1), ("z", 1, 0, 4, 1), ("z", -1, 1, 4, 1), ("z", 1, 2, 4, 1),
    ("z", -1, 3, 4, 1), ("y", 4, 1), ("m", 3, 2, 2), ("y", 3, 2), ("z", 1, 1, 3, 2), ("z", 1, 3, 3, 2),
    ("m", 5, 2, 2), ("y", 5, 2), ("z", -1, 0, 3, 2), ("z", -1, 2, 3, 2), ("m", 2, 2, 2), ("y", 2, 2),
    ("m", 6, 2, 2), ("y", 6, 2), ("z", -1, 1, 3, 2), ("z", 1, 0, 3, 2), ("m", 1, 2, 2), ("y", 1, 2),
    ("z", -1, 5, 4, 2), ("z", 1, 4, 4, 2), ("m", 7, 2, 2), ("y", 7, 2), ("z", -1, 3, 3, 2), ("z", 1, 3, 2, 2),
    ("m", 0, 2, 2), ("z", 1, 1, 2, 2), ("z", -1, 0, 2, 2), ("z", 1, 2, 3, 2), ("b",), ("z", -1, 2, 2, 2),
    ("z", 1, 0, 2, 2), ("z", -1, 1, 2, 2), ("z", 1, 5, 3, 2), ("z", -1, 5, 3, 2), ("z", 1, 4, 3, 2),
    ("z", -1, 4, 3, 2), ("z", 1, 1, 1, 2), ("z", -1, 0, 1, 2), ("z", 1, 2, 2, 2), ("z", -1, 3, 2, 2), ("y", 0, 2),
    ("z", 1, 0, 1, 2), ("z", -1, 1, 1, 2), ("z", 1, 5, 2, 2), ("z", -1, 5, 2, 2), ("z", 1, 4, 2, 2),
    ("z", -1, 4, 2, 2), ("z", 1, 3, 1, 2), ("z", -1, 2, 1, 2), ("z", 1, 2, 1, 2), ("z", -1, 3, 1, 2), ("s", 0),
    ("s", 1), ("z", 1, 5, 1, 2), ("z", -1, 5, 1, 2), ("z", 1, 4, 1, 2), ("z", -1, 4, 1, 2), ("f", 0), ("f", 1),
    ("f", 3), ("f", 2), ("c", 0), ("c", 1), ("c", 3), ("c", 2),
)


def hops(unit, way):
    return 4 if UNITS[unit][3] == way else 3


INBOX = {}
PLACE = {}
for step_ in PLAN:
    if step_[0] == "z":
        INBOX.setdefault((step_[1], step_[2], step_[3] - 1), len(INBOX))
        PLACE[step_[1:]] = len(PLACE)
CROSS = {step_[1:]: i for i, step_ in enumerate(step_ for step_ in PLAN if step_[0] == "y")}
ORDER = (1, 2, 0, 3)


def columns(x):
    at = ORDER.index(x) * LANES
    return slice(at, at + LANES)


def cells(group):
    return (slice(0, 2 * LANES), slice(2 * LANES, CELLS), slice(0, CELLS))[group]


def span(group):
    cols = cells(group)
    return pl.ds(cols.start, cols.stop - cols.start)


def kernel(
    field_in, right_in, mean_in, terms_in, coupling, mask_in, sol, res,
    field, right, mean, terms, mask,
    abuf, lhs_hi, lhs_lo, f_hi, f_lo, part, inbox, ysum, ybox, sbox,
    vp, diffs, base, coef, mrow, cxbox, cybox, mbox, kd, kw, kpack, edge, rowbox, colbox,
    wide, fold, foldbox, corr, direction,
    isem, asem, csend, crecv, msend, mrecv, hsend, hrecv, rsend, rrecv, ysend, yrecv, wsend, wrecv,
):
    mode = lax.axis_index("mode")
    sx = lax.axis_index("sx")
    sy = lax.axis_index("sy")
    z = lax.rem(mode, RING)
    group = lax.div(mode, RING)
    nx, ny = 4, 4
    zp = (group * RING + lax.rem(z + 1, RING), sx, sy)
    zm = (group * RING + lax.rem(z + RING - 1, RING), sx, sy)
    partner = (lax.rem(mode + RING, 2 * RING), sx, sy)
    xp = (mode, lax.rem(sx + 1, nx), sy)
    xm = (mode, lax.rem(sx + nx - 1, nx), sy)
    yp = (mode, sx, lax.rem(sy + 1, ny))
    ym = (mode, sx, lax.rem(sy + ny - 1, ny))
    corners = ((xp[1], yp[2]), (xm[1], yp[2]), (xp[1], ym[2]), (xm[1], ym[2]))
    corners = tuple((mode, i, j) for i, j in corners)

    barrier = pltpu.get_barrier_semaphore()
    peers = (zp, zm, partner, xp, xm, yp, ym) + corners
    for peer in peers:
        pl.semaphore_signal(barrier, inc=1, device_id=peer, device_id_type=MESH)

    fetch = [
        pltpu.make_async_copy(src, dst, isem.at[i])
        for i, (src, dst) in enumerate(
            ((field_in, field), (mean_in, mean), (terms_in, terms), (mask_in, mask), (right_in, right))
        )
    ]
    for copy in fetch:
        copy.start()

    def block_of(o, p):
        owner = group if p == 1 else 1 - group
        return owner * RING + lax.rem(z + o, RING)

    def load(o, p):
        row = pl.multiple_of(block_of(o, p) * ROWS, ROWS)
        return pltpu.make_async_copy(
            coupling.at[:, pl.ds(row, ROWS), :], abuf.at[o * 2 + p], asem.at[o * 2 + p]
        )

    for o in (4, 3, 5, 2, 6, 1, 0, 7):
        for p in (0, 1):
            load(o, p).start()

    lane = lax.broadcasted_iota(jnp.int32, (ROWS, LANES), 1)

    def edges(planes):
        low, high = None, None
        for x in range(WIDE):
            lo_x = planes[x] if x == 0 else pltpu.roll(planes[x], x, 1)
            hi_x = pltpu.roll(planes[x], x + 1, 1)
            low = lo_x if x == 0 else jnp.where(lane == x, lo_x, low)
            high = hi_x if x == 0 else jnp.where(lane == x, hi_x, high)
        for i, value in enumerate((low, high)):
            total = value[0:8]
            for g in range(1, ROWS // 8):
                piece = pltpu.roll(value[g * 8 : (g + 1) * 8], 8 * g, 1)
                total = jnp.where(lane[0:8] >= 8 * g, piece, total)
            edge[i] = total

    def unfolded(box, to, x):
        return jnp.concatenate(
            [pltpu.roll(box, (to - x - 8 * g) % LANES, 1) for g in range(ROWS // 8)], axis=0
        )

    started = []

    def send(src, dst, ssem, rsem, peer):
        copy = pltpu.make_async_remote_copy(
            src_ref=src, dst_ref=dst, send_sem=ssem, recv_sem=rsem, device_id=peer, device_id_type=MESH
        )
        copy.start()
        started.append(copy)
        return copy

    def differences(x):
        center = vp[x]
        up = vp[x - 1] if x > 0 else rowbox[0]
        down = vp[x + 1] if x < WIDE - 1 else rowbox[1]
        lo_col = unfolded(colbox[0], 0, x)
        hi_col = unfolded(colbox[1], LANES - 1, x)
        left = jnp.where(lane == 0, lo_col, pltpu.roll(center, 1, 1))
        after = jnp.where(lane == LANES - 1, hi_col, pltpu.roll(center, LANES - 1, 1))
        return (center - up, center - down, center - left, center - after)

    values = []
    fetch[0].wait()
    for x in range(WIDE):
        plane = field[pl.ds(x, ROWS, stride=WIDE), :]
        vp[x] = plane
        values.append(plane)

    pl.semaphore_wait(barrier, len(peers))

    halo = [
        send(vp.at[WIDE - 1], rowbox.at[0], hsend.at[0], hrecv.at[0], xp),
        send(vp.at[0], rowbox.at[1], hsend.at[1], hrecv.at[1], xm),
    ]
    edges(values)
    halo += [
        send(edge.at[1], colbox.at[0], hsend.at[2], hrecv.at[2], yp),
        send(edge.at[0], colbox.at[1], hsend.at[3], hrecv.at[3], ym),
    ]
    fetch[1].wait()
    fetch[2].wait()
    for x in range(WIDE):
        coef[x] = terms[pl.ds(x, TERMS, stride=WIDE), :]
    mrow[0:WIDE] = mean[...]
    mrow[WIDE:] = mean[...]
    coefs = [
        send(coef, cybox.at[0], csend.at[2], crecv.at[2], yp),
        send(coef, cybox.at[1], csend.at[3], crecv.at[3], ym),
        send(coef.at[WIDE - 1], cxbox.at[0], csend.at[0], crecv.at[0], xp),
        send(coef.at[0], cxbox.at[1], csend.at[1], crecv.at[1], xm),
    ]
    means = [
        send(mrow, mbox.at[i], msend.at[i], mrecv.at[i], peer) for i, peer in enumerate((xp, xm, yp, ym))
    ]
    angles = [
        send(mrow, mbox.at[4 + i], msend.at[4 + i], mrecv.at[4 + i], corner) for i, corner in enumerate(corners)
    ]

    def prepare(o):
        for p in (0, 1):
            load(o, p).wait()
            blk = block_of(o, p)
            for t in range(TERMS):
                value = abuf[o * 2 + p, t] * mask[t, blk, mode].astype(jnp.float32)
                high = value.astype(jnp.bfloat16)
                low = (value - high.astype(jnp.float32)).astype(jnp.bfloat16)
                lhs_hi[o, p * ROWS : (p + 1) * ROWS, t * ROWS : (t + 1) * ROWS] = high
                lhs_lo[o, p * ROWS : (p + 1) * ROWS, t * ROWS : (t + 1) * ROWS] = low

    def multiply(o, parts, groups):
        first, last = parts[0] * ROWS, (parts[-1] + 1) * ROWS
        for group in groups:
            cols = cells(group)
            dot = functools.partial(jnp.dot, preferred_element_type=jnp.float32)
            total = (
                dot(lhs_hi[o, first:last], f_hi[:, cols])
                + dot(lhs_hi[o, first:last], f_lo[:, cols])
                + dot(lhs_lo[o, first:last], f_hi[:, cols])
            )
            for i, p in enumerate(parts):
                part[o, p, :, cols] = total[i * ROWS : (i + 1) * ROWS]

    fetch[3].wait()
    prepare(4)

    def mean_plane(box, x):
        return jnp.broadcast_to(box[x : x + 1, :], (TERMS, LANES))

    thin = lax.broadcasted_iota(jnp.int32, (TERMS, LANES), 1)

    def coefficients(x, rows, own, low, high, before, after):
        up = own(x - 1) if x > 0 else low()
        down = own(x + 1) if x < WIDE - 1 else high()
        here = own(x)
        left = jnp.where(thin == 0, pltpu.roll(before(x), 1, 1), pltpu.roll(here, 1, 1))
        right_of = jnp.where(thin == LANES - 1, pltpu.roll(after(x), LANES - 1, 1), pltpu.roll(here, LANES - 1, 1))
        for d, other in enumerate((up, down, left, right_of)):
            kd[d, x, rows, :] = 0.5 * (here + other)

    def fluxes(copies, planes):
        for copy in copies:
            copy.wait_recv()
        for x in planes:
            coefficients(
                x,
                slice(0, TERMS),
                lambda i: coef[i],
                lambda: cxbox[0],
                lambda: cxbox[1],
                lambda i: cybox[0, i],
                lambda i: cybox[1, i],
            )
            coefficients(
                x,
                slice(TERMS, 2 * TERMS),
                lambda i: mean_plane(mrow, i),
                lambda: mean_plane(mbox.at[0], WIDE - 1),
                lambda: mean_plane(mbox.at[1], 0),
                lambda i: mean_plane(mbox.at[2], i),
                lambda i: mean_plane(mbox.at[3], i),
            )
            for d, delta in enumerate(differences(x)):
                diffs[d, x] = delta

        @pl.loop(0, TERMS)
        def _(t):
            rows = pl.ds(pl.multiple_of(t * ROWS, ROWS), ROWS)
            for x in planes:
                total = None
                for d in range(4):
                    piece = kd[d, x, pl.ds(t, 1), :] * diffs[d, x]
                    total = piece if total is None else total + piece
                high = total.astype(jnp.bfloat16)
                f_hi[rows, columns(x)] = high
                f_lo[rows, columns(x)] = (total - high.astype(jnp.float32)).astype(jnp.bfloat16)

    fluxes(halo[2:] + coefs[:2] + means[2:], (1, 2))

    ring = {}
    crossing = {}
    crossed = set()

    def settle(o):
        if o not in crossed:
            crossed.add(o)
            for copy in crossing[o]:
                copy.wait_recv()
            part[o, 1, CROSSING:, :] += ybox[o]

    def arrived(way, unit, o):
        for copy in ring[(way, unit, o)]:
            copy.wait_recv()

    def forward(way, unit, o, group):
        p, first, count, _ = UNITS[unit]
        at = (o * way) % RING
        if unit >= 4:
            settle(at)
        if o < hops(unit, way):
            arrived(way, unit, o)
            part[at, p, first : first + count, :] += inbox[INBOX[(way, unit, o)], 0:count]
        i = PLACE[(way, unit, o, group)]
        cols = span(group)
        copy = send(
            part.at[at, p, pl.ds(first, count), cols],
            inbox.at[INBOX[(way, unit, o - 1)], pl.ds(0, count), cols],
            rsend.at[i],
            rrecv.at[i],
            zp if way == 1 else zm,
        )
        ring.setdefault((way, unit, o - 1), []).append(copy)

    def collect(unit):
        p, first, count, _ = UNITS[unit]
        for way in (1, -1):
            arrived(way, unit, 0)
        return (
            part[0, p, first : first + count, :]
            + inbox[INBOX[(1, unit, 0)], 0:count]
            + inbox[INBOX[(-1, unit, 0)], 0:count]
        )

    SPAN = WIDE + 2 * SWEEPS
    DEEP = 2 * SWEEPS

    def layout(rows):
        at = lax.broadcasted_iota(jnp.int32, (rows, LANES), 1)
        plane = lax.shift_right_logical(at * 171, 10)
        return at, plane, at - DEEP * plane

    def gather(planes, plane):
        total = None
        for i, value in planes:
            piece = pltpu.roll(value, DEEP * i + SWEEPS, 1)
            total = piece if total is None else jnp.where(plane == i, piece, total)
        return total

    def join(before, own, after, at, column):
        low = jnp.where(column < SWEEPS, before, own)
        high = jnp.where(column < SWEEPS, own, after)
        return jnp.where(at < 64, low, pltpu.roll(high, 64, 1))

    def pack_shifts(pack):
        return (
            pltpu.roll(pack, DEEP, 1),
            pltpu.roll(pack, LANES - DEEP, 1),
            pltpu.roll(pack, 1, 1),
            pltpu.roll(pack, LANES - 1, 1),
        )

    def side_columns(i, value, pack, at):
        left = jnp.where(at == 0, pltpu.roll(pack, LANES - (DEEP * i + SWEEPS - 1), 1), pltpu.roll(value, 1, 1))
        after = jnp.where(
            at == LANES - 1, pltpu.roll(pack, (60 - DEEP * i) % LANES, 1), pltpu.roll(value, LANES - 1, 1)
        )
        return left, after

    def wide_coefficients():
        for copy in angles:
            copy.wait_recv()
        at, plane, column = layout(TERMS)

        def column_of(low, own, high):
            rows = [(i, low(i + 1)) for i in range(SWEEPS)]
            rows += [(SWEEPS + x, own(x)) for x in range(WIDE)]
            return rows + [(SWEEPS + WIDE + i, high(i)) for i in range(SWEEPS)]

        boxes = [mbox.at[i] for i in range(8)]
        here, before, after = (
            column_of(*(functools.partial(mean_plane, box) for box in group))
            for group in (
                (boxes[0], mrow, boxes[1]),
                (boxes[4], boxes[2], boxes[5]),
                (boxes[6], boxes[3], boxes[7]),
            )
        )
        pack = join(gather(before, plane), gather(here, plane), gather(after, plane), at, column)
        for d, other in enumerate(pack_shifts(pack)):
            kpack[d] = 0.5 * (pack + other)
        for i in range(1, SPAN - 1):
            value = here[i][1]
            others = (here[i - 1][1], here[i + 1][1]) + side_columns(i, value, pack, at)
            for d, other in enumerate(others):
                kw[d, i] = 0.5 * (value + other)

    def spread(part_of):
        _, first, count, _ = UNITS[2 + part_of]
        rows = pl.ds(first, count)
        at, plane, _ = layout(count)
        own = gather([(x, wide[SWEEPS + x, rows, :]) for x in range(WIDE)], plane)
        thin_at = at[0:8]
        total = own[0:8]
        for g in range(1, count // 8):
            piece = pltpu.roll(own[g * 8 : (g + 1) * 8], GROUP * g, 1)
            total = jnp.where(thin_at >= GROUP * g, piece, total)
        fold[part_of] = total
        moves = [(fold.at[part_of], foldbox.at[part_of, i], peer) for i, peer in enumerate(corners + (yp, ym))]
        moves += [
            (wide.at[pl.ds(WIDE, SWEEPS), rows, :], wide.at[pl.ds(0, SWEEPS), rows, :], xp),
            (wide.at[pl.ds(SWEEPS, SWEEPS), rows, :], wide.at[pl.ds(SWEEPS + WIDE, SWEEPS), rows, :], xm),
        ]
        return [
            send(src, dst, wsend.at[part_of, i], wrecv.at[part_of, i], peer)
            for i, (src, dst, peer) in enumerate(moves)
        ]

    def sweeps(part_of, moved):
        for copy in moved:
            copy.wait_recv()
        _, first, count, _ = UNITS[2 + part_of]
        rows = pl.ds(first, count)
        at, plane, column = layout(count)

        def unfold(i, shift):
            return jnp.concatenate(
                [pltpu.roll(foldbox[part_of, i], (shift - GROUP * g) % LANES, 1) for g in range(count // 8)], axis=0
            )

        def beside(low, mid, high):
            total = jnp.where(plane < SWEEPS, unfold(low, -DEEP), unfold(mid, DEEP * SWEEPS))
            return jnp.where(plane >= SWEEPS + WIDE, unfold(high, DEEP * (SWEEPS + WIDE)), total)

        here = [(i, wide[i, rows, :]) for i in range(SPAN)]
        pack = join(beside(0, 4, 1), gather(here, plane), beside(2, 5, 3), at, column)
        wide[SPAN, rows, :] = pack
        for i in range(SPAN + 1):
            value = wide[i, rows, :] * (1.0 / THETA)
            corr[0, i, rows, :] = value
            direction[i, rows, :] = value

        sigma = THETA / DELTA
        rho = 1.0 / sigma
        for sweep in range(SWEEPS):
            now, later = sweep % 2, (sweep + 1) % 2
            rho_next = 1.0 / (2.0 * sigma - rho)
            pack = corr[now, SPAN, rows, :]

            def advance(i, value, others, coefficients):
                applied = REACT * value
                for d in range(4):
                    applied = applied + coefficients(d) * (value - others[d])
                step = rho_next * rho * direction[i, rows, :]
                step = step + (2.0 * rho_next / DELTA) * (wide[i, rows, :] - applied)
                return step

            for i in range(sweep + 1, SPAN - 1 - sweep):
                value = corr[now, i, rows, :]
                others = (corr[now, i - 1, rows, :], corr[now, i + 1, rows, :]) + side_columns(i, value, pack, at)
                step = advance(i, value, others, lambda d: kw[d, i, 0:1, :])
                if sweep < SWEEPS - 1:
                    direction[i, rows, :] = step
                    corr[later, i, rows, :] = value + step
                else:
                    x = i - SWEEPS
                    sol[pl.ds(first * WIDE + x, count, stride=WIDE), :] = vp[x, rows, :] + (value + step)
            if sweep < SWEEPS - 1:
                step = advance(SPAN, pack, pack_shifts(pack), lambda d: kpack[d, 0:1, :])
                direction[SPAN, rows, :] = step
                corr[later, SPAN, rows, :] = pack + step
            rho = rho_next

    def prepare_residual():
        fetch[4].wait()
        for x in range(WIDE):
            total = REACT * vp[x]
            for d in range(4):
                total = total + kd[d, x, TERMS : TERMS + 1, :] * diffs[d, x]
            base[x] = right[pl.ds(x, ROWS, stride=WIDE), :] - total
        wide_coefficients()

    sums = {}

    def finish(quarter):
        _, first, count, _ = UNITS[2 + quarter]
        rows = slice(first, first + count)
        if quarter in sums:
            sums[quarter].wait_recv()
            total = collect(2 + quarter) + sbox[rows]
        else:
            settle(0)
            total = collect(2 + quarter)
        for x in range(WIDE):
            value = base[x, rows, :] - total[:, columns(x)]
            wide[SWEEPS + x, rows, :] = value
            res[pl.ds(first * WIDE + x, count, stride=WIDE), :] = value
        return spread(quarter)

    spreads = {}
    for step in PLAN:
        what = step[0]
        if what == "m":
            if step[1] != 4:
                prepare(step[1])
            multiply(step[1], ((0,), (1,), (0, 1))[step[2]], ((0,), (1,), (0, 1))[step[3]])
        elif what == "z":
            forward(*step[1:])
        elif what == "y":
            o, cols, i = step[1], span(step[2]), CROSS[step[1:]]
            copy = send(
                part.at[o, 0, pl.ds(CROSSING, ROWS - CROSSING), cols], ybox.at[o, :, cols], ysend.at[i], yrecv.at[i], partner
            )
            crossing.setdefault(o, []).append(copy)
        elif what == "s":
            i = step[1]
            rows = pl.ds(UNITS[i][1], UNITS[i][2])
            ysum[rows, :] = collect(i)
            sums[i] = send(ysum.at[rows], sbox.at[rows], ysend.at[len(CROSS) + i], yrecv.at[len(CROSS) + i], partner)
        elif what == "x":
            fluxes(halo[:2] + coefs[2:] + means[:2], (0, 3))
        elif what == "b":
            prepare_residual()
        elif what == "f":
            spreads[step[1]] = finish(step[1])
        else:
            sweeps(step[1], spreads[step[1]])

    for copy in started:
        copy.wait_send()


def place(sol, res, sol_out, res_out, sem):
    copies = [pltpu.make_async_copy(sol, sol_out, sem.at[0]), pltpu.make_async_copy(res, res_out, sem.at[1])]
    for copy in copies:
        copy.start()
    for copy in copies:
        copy.wait()


def local(start_field, right_side, mean_coef, term_coef, coupling, block_mask):
    modes, wide, lanes = start_field.shape
    f32, bf16 = jnp.float32, jnp.bfloat16
    vmem = pl.BlockSpec(memory_space=pltpu.VMEM)
    flat = jax.ShapeDtypeStruct((modes * wide, lanes), f32)
    sol, res = pl.pallas_call(
        kernel,
        out_shape=(flat, flat),
        in_specs=[pl.BlockSpec(memory_space=pltpu.HBM)] * 6,
        out_specs=(vmem, vmem),
        scratch_shapes=[
            pltpu.VMEM((modes * wide, lanes), f32),
            pltpu.VMEM((modes * wide, lanes), f32),
            pltpu.VMEM(mean_coef.shape, f32),
            pltpu.VMEM((TERMS * WIDE, lanes), f32),
            pltpu.SMEM(block_mask.shape, jnp.int32),
            pltpu.VMEM((2 * RING, TERMS, ROWS, ROWS), f32),
            pltpu.VMEM((RING, 2 * ROWS, TERMS * ROWS), bf16),
            pltpu.VMEM((RING, 2 * ROWS, TERMS * ROWS), bf16),
            pltpu.VMEM((TERMS * ROWS, CELLS), bf16),
            pltpu.VMEM((TERMS * ROWS, CELLS), bf16),
            pltpu.VMEM((RING, 2, ROWS, CELLS), f32),
            pltpu.VMEM((len(INBOX), MOST, CELLS), f32),
            pltpu.VMEM((CROSSING, CELLS), f32),
            pltpu.VMEM((RING, ROWS - CROSSING, CELLS), f32),
            pltpu.VMEM((CROSSING, CELLS), f32),
            pltpu.VMEM((WIDE, ROWS, LANES), f32),
            pltpu.VMEM((4, WIDE, ROWS, LANES), f32),
            pltpu.VMEM((WIDE, ROWS, LANES), f32),
            pltpu.VMEM((WIDE, TERMS, LANES), f32),
            pltpu.VMEM((TERMS, LANES), f32),
            pltpu.VMEM((2, TERMS, LANES), f32),
            pltpu.VMEM((2, WIDE, TERMS, LANES), f32),
            pltpu.VMEM((8, TERMS, LANES), f32),
            pltpu.VMEM((4, WIDE, 2 * TERMS, LANES), f32),
            pltpu.VMEM((4, WIDE + 2 * SWEEPS, TERMS, LANES), f32),
            pltpu.VMEM((4, TERMS, LANES), f32),
            pltpu.VMEM((2, 8, LANES), f32),
            pltpu.VMEM((2, ROWS, LANES), f32),
            pltpu.VMEM((2, 8, LANES), f32),
            pltpu.VMEM((WIDE + 2 * SWEEPS + 1, ROWS, LANES), f32),
            pltpu.VMEM((4, 8, LANES), f32),
            pltpu.VMEM((4, 6, 8, LANES), f32),
            pltpu.VMEM((2, WIDE + 2 * SWEEPS + 1, ROWS, LANES), f32),
            pltpu.VMEM((WIDE + 2 * SWEEPS + 1, ROWS, LANES), f32),
            pltpu.SemaphoreType.DMA((5,)),
            pltpu.SemaphoreType.DMA((2 * RING,)),
            pltpu.SemaphoreType.DMA((4,)),
            pltpu.SemaphoreType.DMA((4,)),
            pltpu.SemaphoreType.DMA((8,)),
            pltpu.SemaphoreType.DMA((8,)),
            pltpu.SemaphoreType.DMA((4,)),
            pltpu.SemaphoreType.DMA((4,)),
            pltpu.SemaphoreType.DMA((len(PLACE),)),
            pltpu.SemaphoreType.DMA((len(PLACE),)),
            pltpu.SemaphoreType.DMA((len(CROSS) + 2,)),
            pltpu.SemaphoreType.DMA((len(CROSS) + 2,)),
            pltpu.SemaphoreType.DMA((4, 8)),
            pltpu.SemaphoreType.DMA((4, 8)),
        ],
        compiler_params=pltpu.CompilerParams(
            collective_id=0, has_side_effects=True, vmem_limit_bytes=48000 * 1024
        ),
        name="galerkin_step",
    )(
        *(
            pltpu.with_memory_space_constraint(value, pltpu.HBM)
            for value in (
                start_field.reshape(modes * wide, lanes),
                right_side.reshape(modes * wide, lanes),
                mean_coef,
                term_coef.reshape(-1, lanes),
                coupling,
                block_mask,
            )
        )
    )
    hbm = pl.BlockSpec(memory_space=pltpu.HBM)
    sol, res = pl.pallas_call(
        place,
        out_shape=(flat, flat),
        in_specs=[vmem, vmem],
        out_specs=(hbm, hbm),
        scratch_shapes=[pltpu.SemaphoreType.DMA((2,))],
        compiler_params=pltpu.CompilerParams(vmem_limit_bytes=1 << 20),
        name="place",
    )(sol, res)
    return (sol.reshape(start_field.shape), res.reshape(start_field.shape))


def solution(mesh):
    placed = (
        P("mode", "sx", "sy"),
        P("mode", "sx", "sy"),
        P("sx", "sy"),
        P(None, "sx", "sy"),
        P(None, None, "mode"),
        P(),
    )
    return jax.shard_map(
        local,
        mesh=mesh,
        in_specs=placed,
        out_specs=(P("mode", "sx", "sy"), P("mode", "sx", "sy")),
        check_vma=False,
    )
```

```python
import functools

import jax
import jax.numpy as jnp
from jax import lax
from jax.experimental import pallas as pl
from jax.experimental.pallas import tpu as pltpu
from jax.sharding import PartitionSpec as P

SWEEPS = 3
REACT = 0.5
THETA = 8.5
DELTA = 8.0
MESH = pl.DeviceIdType.MESH
RING = 8
GROUPS = 2
ROWS = 128
WIDE = 4
LANES = 128
CELLS = WIDE * LANES
TERMS = 8

EARLY = (32, 24)
LATE = (32, 40)
CROSSING = sum(EARLY)
UNITS = tuple(
    (p, first + (rows[0] if way < 0 else 0), rows[way < 0], way)
    for p, first, rows in ((0, 0, EARLY), (1, 0, EARLY), (1, CROSSING, LATE))
    for way in (1, -1)
)
MOST = max(EARLY + LATE)
GROUP = WIDE * 2 * SWEEPS

PLAN = (
    ("m", 4, 0, 0), ("z", 1, 0, 4, 0), ("z", -1, 1, 4, 0), ("y", 4, 0), ("m", 4, 1, 0), ("z", 1, 2, 4, 0),
    ("z", -1, 3, 4, 0), ("x",), ("m", 4, 2, 1), ("z", 1, 0, 4, 1), ("z", -1, 1, 4, 1), ("z", 1, 2, 4, 1),
    ("z", -1, 3, 4, 1), ("y", 4, 1), ("m", 3, 2, 2), ("y", 3, 2), ("z", 1, 1, 3, 2), ("z", 1, 3, 3, 2),
    ("m", 5, 2, 2), ("y", 5, 2), ("z", -1, 0, 3, 2), ("z", -1, 2, 3, 2), ("m", 2, 2, 2), ("y", 2, 2),
    ("m", 6, 2, 2), ("y", 6, 2), ("z", 1, 0, 3, 2), ("z", -1, 1, 3, 2), ("m", 1, 2, 2), ("y", 1, 2),
    ("z", -1, 5, 4, 2), ("z", 1, 4, 4, 2), ("m", 7, 2, 2), ("y", 7, 2), ("z", 1, 1, 2, 2), ("z", -1, 3, 3, 2),
    ("z", 1, 3, 2, 2), ("m", 0, 2, 2), ("z", 1, 2, 3, 2), ("z", -1, 0, 2, 2), ("b",), ("z", -1, 2, 2, 2),
    ("z", 1, 0, 2, 2), ("z", -1, 1, 2, 2), ("z", 1, 5, 3, 2), ("z", -1, 5, 3, 2), ("z", 1, 1, 1, 2),
    ("z", -1, 4, 3, 2), ("z", 1, 4, 3, 2), ("z", -1, 0, 1, 2), ("z", 1, 2, 2, 2), ("z", -1, 3, 2, 2),
    ("z", 1, 0, 1, 2), ("z", -1, 1, 1, 2), ("z", 1, 5, 2, 2), ("y", 0, 2), ("z", -1, 5, 2, 2), ("z", 1, 3, 1, 2),
    ("z", -1, 4, 2, 2), ("z", 1, 4, 2, 2), ("z", -1, 2, 1, 2), ("z", 1, 2, 1, 2), ("s", 0), ("z", -1, 3, 1, 2),
    ("s", 1), ("z", 1, 5, 1, 2), ("z", -1, 5, 1, 2), ("z", -1, 4, 1, 2), ("z", 1, 4, 1, 2), ("f", 0), ("f", 1),
    ("f", 3), ("f", 2), ("c", 0), ("c", 1), ("c", 3), ("c", 2),
)


def hops(unit, way):
    return 4 if UNITS[unit][3] == way else 3


INBOX = {}
PLACE = {}
for step_ in PLAN:
    if step_[0] == "z":
        INBOX.setdefault((step_[1], step_[2], step_[3] - 1), len(INBOX))
        PLACE[step_[1:]] = len(PLACE)
CROSS = {step_[1:]: i for i, step_ in enumerate(step_ for step_ in PLAN if step_[0] == "y")}
ORDER = (1, 2, 0, 3)


def columns(x):
    at = ORDER.index(x) * LANES
    return slice(at, at + LANES)


def cells(group):
    return (slice(0, 2 * LANES), slice(2 * LANES, CELLS), slice(0, CELLS))[group]


def span(group):
    cols = cells(group)
    return pl.ds(cols.start, cols.stop - cols.start)


def kernel(
    field_in, right_in, mean_in, terms_in, coupling, mask_in, sol, res,
    field, right, mean, terms, mask,
    abuf, lhs_hi, lhs_lo, f_hi, f_lo, part, inbox, ysum, ybox, sbox,
    vp, diffs, base, coef, mrow, cxbox, cybox, mbox, kd, kw, kpack, edge, rowbox, colbox,
    wide, fold, foldbox, corr, direction,
    isem, asem, csend, crecv, msend, mrecv, hsend, hrecv, rsend, rrecv, ysend, yrecv, wsend, wrecv,
):
    mode = lax.axis_index("mode")
    sx = lax.axis_index("sx")
    sy = lax.axis_index("sy")
    z = lax.rem(mode, RING)
    group = lax.div(mode, RING)
    nx, ny = 4, 4
    zp = (group * RING + lax.rem(z + 1, RING), sx, sy)
    zm = (group * RING + lax.rem(z + RING - 1, RING), sx, sy)
    partner = (lax.rem(mode + RING, 2 * RING), sx, sy)
    xp = (mode, lax.rem(sx + 1, nx), sy)
    xm = (mode, lax.rem(sx + nx - 1, nx), sy)
    yp = (mode, sx, lax.rem(sy + 1, ny))
    ym = (mode, sx, lax.rem(sy + ny - 1, ny))
    corners = ((xp[1], yp[2]), (xm[1], yp[2]), (xp[1], ym[2]), (xm[1], ym[2]))
    corners = tuple((mode, i, j) for i, j in corners)

    barrier = pltpu.get_barrier_semaphore()
    peers = (zp, zm, partner, xp, xm, yp, ym) + corners
    for peer in peers:
        pl.semaphore_signal(barrier, inc=1, device_id=peer, device_id_type=MESH)

    fetch = [
        pltpu.make_async_copy(src, dst, isem.at[i])
        for i, (src, dst) in enumerate(
            ((field_in, field), (mean_in, mean), (terms_in, terms), (mask_in, mask), (right_in, right))
        )
    ]
    for copy in fetch:
        copy.start()

    def block_of(o, p):
        owner = group if p == 1 else 1 - group
        return owner * RING + lax.rem(z + o, RING)

    def load(o, p):
        row = pl.multiple_of(block_of(o, p) * ROWS, ROWS)
        return pltpu.make_async_copy(
            coupling.at[:, pl.ds(row, ROWS), :], abuf.at[o * 2 + p], asem.at[o * 2 + p]
        )

    for o in (4, 3, 5, 2, 6, 1, 0, 7):
        for p in (0, 1):
            load(o, p).start()

    lane = lax.broadcasted_iota(jnp.int32, (ROWS, LANES), 1)

    def edges(planes):
        low, high = None, None
        for x in range(WIDE):
            lo_x = planes[x] if x == 0 else pltpu.roll(planes[x], x, 1)
            hi_x = pltpu.roll(planes[x], x + 1, 1)
            low = lo_x if x == 0 else jnp.where(lane == x, lo_x, low)
            high = hi_x if x == 0 else jnp.where(lane == x, hi_x, high)
        for i, value in enumerate((low, high)):
            total = value[0:8]
            for g in range(1, ROWS // 8):
                piece = pltpu.roll(value[g * 8 : (g + 1) * 8], 8 * g, 1)
                total = jnp.where(lane[0:8] >= 8 * g, piece, total)
            edge[i] = total

    def unfolded(box, to, x):
        return jnp.concatenate(
            [pltpu.roll(box, (to - x - 8 * g) % LANES, 1) for g in range(ROWS // 8)], axis=0
        )

    started = []

    def send(src, dst, ssem, rsem, peer):
        copy = pltpu.make_async_remote_copy(
            src_ref=src, dst_ref=dst, send_sem=ssem, recv_sem=rsem, device_id=peer, device_id_type=MESH
        )
        copy.start()
        started.append(copy)
        return copy

    def differences(x):
        center = vp[x]
        up = vp[x - 1] if x > 0 else rowbox[0]
        down = vp[x + 1] if x < WIDE - 1 else rowbox[1]
        lo_col = unfolded(colbox[0], 0, x)
        hi_col = unfolded(colbox[1], LANES - 1, x)
        left = jnp.where(lane == 0, lo_col, pltpu.roll(center, 1, 1))
        after = jnp.where(lane == LANES - 1, hi_col, pltpu.roll(center, LANES - 1, 1))
        return (center - up, center - down, center - left, center - after)

    values = []
    fetch[0].wait()
    for x in range(WIDE):
        plane = field[pl.ds(x, ROWS, stride=WIDE), :]
        vp[x] = plane
        values.append(plane)

    pl.semaphore_wait(barrier, len(peers))

    halo = [
        send(vp.at[WIDE - 1], rowbox.at[0], hsend.at[0], hrecv.at[0], xp),
        send(vp.at[0], rowbox.at[1], hsend.at[1], hrecv.at[1], xm),
    ]
    edges(values)
    halo += [
        send(edge.at[1], colbox.at[0], hsend.at[2], hrecv.at[2], yp),
        send(edge.at[0], colbox.at[1], hsend.at[3], hrecv.at[3], ym),
    ]
    fetch[1].wait()
    fetch[2].wait()
    for x in range(WIDE):
        coef[x] = terms[pl.ds(x, TERMS, stride=WIDE), :]
    mrow[0:WIDE] = mean[...]
    mrow[WIDE:] = mean[...]
    coefs = [
        send(coef, cybox.at[0], csend.at[2], crecv.at[2], yp),
        send(coef, cybox.at[1], csend.at[3], crecv.at[3], ym),
        send(coef.at[WIDE - 1], cxbox.at[0], csend.at[0], crecv.at[0], xp),
        send(coef.at[0], cxbox.at[1], csend.at[1], crecv.at[1], xm),
    ]
    means = [
        send(mrow, mbox.at[i], msend.at[i], mrecv.at[i], peer) for i, peer in enumerate((xp, xm, yp, ym))
    ]
    angles = [
        send(mrow, mbox.at[4 + i], msend.at[4 + i], mrecv.at[4 + i], corner) for i, corner in enumerate(corners)
    ]

    def prepare(o):
        for p in (0, 1):
            load(o, p).wait()
            blk = block_of(o, p)
            for t in range(TERMS):
                value = abuf[o * 2 + p, t] * mask[t, blk, mode].astype(jnp.float32)
                high = value.astype(jnp.bfloat16)
                low = (value - high.astype(jnp.float32)).astype(jnp.bfloat16)
                lhs_hi[o, p * ROWS : (p + 1) * ROWS, t * ROWS : (t + 1) * ROWS] = high
                lhs_lo[o, p * ROWS : (p + 1) * ROWS, t * ROWS : (t + 1) * ROWS] = low

    def multiply(o, parts, groups):
        first, last = parts[0] * ROWS, (parts[-1] + 1) * ROWS
        for group in groups:
            cols = cells(group)
            dot = functools.partial(jnp.dot, preferred_element_type=jnp.float32)
            total = (
                dot(lhs_hi[o, first:last], f_hi[:, cols])
                + dot(lhs_hi[o, first:last], f_lo[:, cols])
                + dot(lhs_lo[o, first:last], f_hi[:, cols])
            )
            for i, p in enumerate(parts):
                part[o, p, :, cols] = total[i * ROWS : (i + 1) * ROWS]

    fetch[3].wait()
    prepare(4)

    def mean_plane(box, x):
        return jnp.broadcast_to(box[x : x + 1, :], (TERMS, LANES))

    thin = lax.broadcasted_iota(jnp.int32, (TERMS, LANES), 1)

    def coefficients(x, rows, own, low, high, before, after):
        up = own(x - 1) if x > 0 else low()
        down = own(x + 1) if x < WIDE - 1 else high()
        here = own(x)
        left = jnp.where(thin == 0, pltpu.roll(before(x), 1, 1), pltpu.roll(here, 1, 1))
        right_of = jnp.where(thin == LANES - 1, pltpu.roll(after(x), LANES - 1, 1), pltpu.roll(here, LANES - 1, 1))
        for d, other in enumerate((up, down, left, right_of)):
            kd[d, x, rows, :] = 0.5 * (here + other)

    def fluxes(copies, planes):
        for copy in copies:
            copy.wait_recv()
        for x in planes:
            coefficients(
                x,
                slice(0, TERMS),
                lambda i: coef[i],
                lambda: cxbox[0],
                lambda: cxbox[1],
                lambda i: cybox[0, i],
                lambda i: cybox[1, i],
            )
            coefficients(
                x,
                slice(TERMS, 2 * TERMS),
                lambda i: mean_plane(mrow, i),
                lambda: mean_plane(mbox.at[0], WIDE - 1),
                lambda: mean_plane(mbox.at[1], 0),
                lambda i: mean_plane(mbox.at[2], i),
                lambda i: mean_plane(mbox.at[3], i),
            )
            for d, delta in enumerate(differences(x)):
                diffs[d, x] = delta

        @pl.loop(0, TERMS)
        def _(t):
            rows = pl.ds(pl.multiple_of(t * ROWS, ROWS), ROWS)
            for x in planes:
                total = None
                for d in range(4):
                    piece = kd[d, x, pl.ds(t, 1), :] * diffs[d, x]
                    total = piece if total is None else total + piece
                high = total.astype(jnp.bfloat16)
                f_hi[rows, columns(x)] = high
                f_lo[rows, columns(x)] = (total - high.astype(jnp.float32)).astype(jnp.bfloat16)

    fluxes(halo[2:] + coefs[:2] + means[2:], (1, 2))

    ring = {}
    crossing = {}
    crossed = set()

    def settle(o):
        if o not in crossed:
            crossed.add(o)
            for copy in crossing[o]:
                copy.wait_recv()
            part[o, 1, CROSSING:, :] += ybox[o]

    def arrived(way, unit, o):
        for copy in ring[(way, unit, o)]:
            copy.wait_recv()

    def forward(way, unit, o, group):
        p, first, count, _ = UNITS[unit]
        at = (o * way) % RING
        if unit >= 4:
            settle(at)
        if o < hops(unit, way):
            arrived(way, unit, o)
            part[at, p, first : first + count, :] += inbox[INBOX[(way, unit, o)], 0:count]
        i = PLACE[(way, unit, o, group)]
        cols = span(group)
        copy = send(
            part.at[at, p, pl.ds(first, count), cols],
            inbox.at[INBOX[(way, unit, o - 1)], pl.ds(0, count), cols],
            rsend.at[i],
            rrecv.at[i],
            zp if way == 1 else zm,
        )
        ring.setdefault((way, unit, o - 1), []).append(copy)

    def collect(unit):
        p, first, count, _ = UNITS[unit]
        for way in (1, -1):
            arrived(way, unit, 0)
        return (
            part[0, p, first : first + count, :]
            + inbox[INBOX[(1, unit, 0)], 0:count]
            + inbox[INBOX[(-1, unit, 0)], 0:count]
        )

    SPAN = WIDE + 2 * SWEEPS
    DEEP = 2 * SWEEPS

    def layout(rows):
        at = lax.broadcasted_iota(jnp.int32, (rows, LANES), 1)
        plane = lax.shift_right_logical(at * 171, 10)
        return at, plane, at - DEEP * plane

    def gather(planes, plane):
        total = None
        for i, value in planes:
            piece = pltpu.roll(value, DEEP * i + SWEEPS, 1)
            total = piece if total is None else jnp.where(plane == i, piece, total)
        return total

    def join(before, own, after, at, column):
        low = jnp.where(column < SWEEPS, before, own)
        high = jnp.where(column < SWEEPS, own, after)
        return jnp.where(at < 64, low, pltpu.roll(high, 64, 1))

    def pack_shifts(pack):
        return (
            pltpu.roll(pack, DEEP, 1),
            pltpu.roll(pack, LANES - DEEP, 1),
            pltpu.roll(pack, 1, 1),
            pltpu.roll(pack, LANES - 1, 1),
        )

    def side_columns(i, value, pack, at):
        left = jnp.where(at == 0, pltpu.roll(pack, LANES - (DEEP * i + SWEEPS - 1), 1), pltpu.roll(value, 1, 1))
        after = jnp.where(
            at == LANES - 1, pltpu.roll(pack, (60 - DEEP * i) % LANES, 1), pltpu.roll(value, LANES - 1, 1)
        )
        return left, after

    def wide_coefficients():
        for copy in angles:
            copy.wait_recv()
        at, plane, column = layout(TERMS)

        def column_of(low, own, high):
            rows = [(i, low(i + 1)) for i in range(SWEEPS)]
            rows += [(SWEEPS + x, own(x)) for x in range(WIDE)]
            return rows + [(SWEEPS + WIDE + i, high(i)) for i in range(SWEEPS)]

        boxes = [mbox.at[i] for i in range(8)]
        here, before, after = (
            column_of(*(functools.partial(mean_plane, box) for box in group))
            for group in (
                (boxes[0], mrow, boxes[1]),
                (boxes[4], boxes[2], boxes[5]),
                (boxes[6], boxes[3], boxes[7]),
            )
        )
        pack = join(gather(before, plane), gather(here, plane), gather(after, plane), at, column)
        for d, other in enumerate(pack_shifts(pack)):
            kpack[d] = 0.5 * (pack + other)
        for i in range(1, SPAN - 1):
            value = here[i][1]
            others = (here[i - 1][1], here[i + 1][1]) + side_columns(i, value, pack, at)
            for d, other in enumerate(others):
                kw[d, i] = 0.5 * (value + other)

    def spread(part_of):
        _, first, count, _ = UNITS[2 + part_of]
        rows = pl.ds(first, count)
        at, plane, _ = layout(count)
        own = gather([(x, wide[SWEEPS + x, rows, :]) for x in range(WIDE)], plane)
        thin_at = at[0:8]
        total = own[0:8]
        for g in range(1, count // 8):
            piece = pltpu.roll(own[g * 8 : (g + 1) * 8], GROUP * g, 1)
            total = jnp.where(thin_at >= GROUP * g, piece, total)
        fold[part_of] = total
        moves = [(fold.at[part_of], foldbox.at[part_of, i], peer) for i, peer in enumerate(corners + (yp, ym))]
        moves += [
            (wide.at[pl.ds(WIDE, SWEEPS), rows, :], wide.at[pl.ds(0, SWEEPS), rows, :], xp),
            (wide.at[pl.ds(SWEEPS, SWEEPS), rows, :], wide.at[pl.ds(SWEEPS + WIDE, SWEEPS), rows, :], xm),
        ]
        return [
            send(src, dst, wsend.at[part_of, i], wrecv.at[part_of, i], peer)
            for i, (src, dst, peer) in enumerate(moves)
        ]

    def sweeps(part_of, moved):
        for copy in moved:
            copy.wait_recv()
        _, first, count, _ = UNITS[2 + part_of]
        rows = pl.ds(first, count)
        at, plane, column = layout(count)

        def unfold(i, shift):
            return jnp.concatenate(
                [pltpu.roll(foldbox[part_of, i], (shift - GROUP * g) % LANES, 1) for g in range(count // 8)], axis=0
            )

        def beside(low, mid, high):
            total = jnp.where(plane < SWEEPS, unfold(low, -DEEP), unfold(mid, DEEP * SWEEPS))
            return jnp.where(plane >= SWEEPS + WIDE, unfold(high, DEEP * (SWEEPS + WIDE)), total)

        here = [(i, wide[i, rows, :]) for i in range(SPAN)]
        pack = join(beside(0, 4, 1), gather(here, plane), beside(2, 5, 3), at, column)
        wide[SPAN, rows, :] = pack
        for i in range(SPAN + 1):
            value = wide[i, rows, :] * (1.0 / THETA)
            corr[0, i, rows, :] = value
            direction[i, rows, :] = value

        sigma = THETA / DELTA
        rho = 1.0 / sigma
        for sweep in range(SWEEPS):
            now, later = sweep % 2, (sweep + 1) % 2
            rho_next = 1.0 / (2.0 * sigma - rho)
            pack = corr[now, SPAN, rows, :]

            def advance(i, value, others, coefficients):
                applied = REACT * value
                for d in range(4):
                    applied = applied + coefficients(d) * (value - others[d])
                step = rho_next * rho * direction[i, rows, :]
                step = step + (2.0 * rho_next / DELTA) * (wide[i, rows, :] - applied)
                return step

            for i in range(sweep + 1, SPAN - 1 - sweep):
                value = corr[now, i, rows, :]
                others = (corr[now, i - 1, rows, :], corr[now, i + 1, rows, :]) + side_columns(i, value, pack, at)
                step = advance(i, value, others, lambda d: kw[d, i, 0:1, :])
                if sweep < SWEEPS - 1:
                    direction[i, rows, :] = step
                    corr[later, i, rows, :] = value + step
                else:
                    x = i - SWEEPS
                    sol[pl.ds(first * WIDE + x, count, stride=WIDE), :] = vp[x, rows, :] + (value + step)
            if sweep < SWEEPS - 1:
                step = advance(SPAN, pack, pack_shifts(pack), lambda d: kpack[d, 0:1, :])
                direction[SPAN, rows, :] = step
                corr[later, SPAN, rows, :] = pack + step
            rho = rho_next

    def prepare_residual():
        fetch[4].wait()
        for x in range(WIDE):
            total = REACT * vp[x]
            for d in range(4):
                total = total + kd[d, x, TERMS : TERMS + 1, :] * diffs[d, x]
            base[x] = right[pl.ds(x, ROWS, stride=WIDE), :] - total
        wide_coefficients()

    sums = {}

    def finish(quarter):
        _, first, count, _ = UNITS[2 + quarter]
        rows = slice(first, first + count)
        if quarter in sums:
            sums[quarter].wait_recv()
            total = collect(2 + quarter) + sbox[rows]
        else:
            settle(0)
            total = collect(2 + quarter)
        for x in range(WIDE):
            value = base[x, rows, :] - total[:, columns(x)]
            wide[SWEEPS + x, rows, :] = value
            res[pl.ds(first * WIDE + x, count, stride=WIDE), :] = value
        return spread(quarter)

    spreads = {}
    for step in PLAN:
        what = step[0]
        if what == "m":
            if step[1] != 4:
                prepare(step[1])
            multiply(step[1], ((0,), (1,), (0, 1))[step[2]], ((0,), (1,), (0, 1))[step[3]])
        elif what == "z":
            forward(*step[1:])
        elif what == "y":
            o, cols, i = step[1], span(step[2]), CROSS[step[1:]]
            copy = send(
                part.at[o, 0, pl.ds(CROSSING, ROWS - CROSSING), cols], ybox.at[o, :, cols], ysend.at[i], yrecv.at[i], partner
            )
            crossing.setdefault(o, []).append(copy)
        elif what == "s":
            i = step[1]
            rows = pl.ds(UNITS[i][1], UNITS[i][2])
            ysum[rows, :] = collect(i)
            sums[i] = send(ysum.at[rows], sbox.at[rows], ysend.at[len(CROSS) + i], yrecv.at[len(CROSS) + i], partner)
        elif what == "x":
            fluxes(halo[:2] + coefs[2:] + means[:2], (0, 3))
        elif what == "b":
            prepare_residual()
        elif what == "f":
            spreads[step[1]] = finish(step[1])
        else:
            sweeps(step[1], spreads[step[1]])

    for copy in started:
        copy.wait_send()


def place(sol, res, sol_out, res_out, sem):
    copies = [pltpu.make_async_copy(sol, sol_out, sem.at[0]), pltpu.make_async_copy(res, res_out, sem.at[1])]
    for copy in copies:
        copy.start()
    for copy in copies:
        copy.wait()


def local(start_field, right_side, mean_coef, term_coef, coupling, block_mask):
    modes, wide, lanes = start_field.shape
    f32, bf16 = jnp.float32, jnp.bfloat16
    vmem = pl.BlockSpec(memory_space=pltpu.VMEM)
    flat = jax.ShapeDtypeStruct((modes * wide, lanes), f32)
    sol, res = pl.pallas_call(
        kernel,
        out_shape=(flat, flat),
        in_specs=[pl.BlockSpec(memory_space=pltpu.HBM)] * 6,
        out_specs=(vmem, vmem),
        scratch_shapes=[
            pltpu.VMEM((modes * wide, lanes), f32),
            pltpu.VMEM((modes * wide, lanes), f32),
            pltpu.VMEM(mean_coef.shape, f32),
            pltpu.VMEM((TERMS * WIDE, lanes), f32),
            pltpu.SMEM(block_mask.shape, jnp.int32),
            pltpu.VMEM((2 * RING, TERMS, ROWS, ROWS), f32),
            pltpu.VMEM((RING, 2 * ROWS, TERMS * ROWS), bf16),
            pltpu.VMEM((RING, 2 * ROWS, TERMS * ROWS), bf16),
            pltpu.VMEM((TERMS * ROWS, CELLS), bf16),
            pltpu.VMEM((TERMS * ROWS, CELLS), bf16),
            pltpu.VMEM((RING, 2, ROWS, CELLS), f32),
            pltpu.VMEM((len(INBOX), MOST, CELLS), f32),
            pltpu.VMEM((CROSSING, CELLS), f32),
            pltpu.VMEM((RING, ROWS - CROSSING, CELLS), f32),
            pltpu.VMEM((CROSSING, CELLS), f32),
            pltpu.VMEM((WIDE, ROWS, LANES), f32),
            pltpu.VMEM((4, WIDE, ROWS, LANES), f32),
            pltpu.VMEM((WIDE, ROWS, LANES), f32),
            pltpu.VMEM((WIDE, TERMS, LANES), f32),
            pltpu.VMEM((TERMS, LANES), f32),
            pltpu.VMEM((2, TERMS, LANES), f32),
            pltpu.VMEM((2, WIDE, TERMS, LANES), f32),
            pltpu.VMEM((8, TERMS, LANES), f32),
            pltpu.VMEM((4, WIDE, 2 * TERMS, LANES), f32),
            pltpu.VMEM((4, WIDE + 2 * SWEEPS, TERMS, LANES), f32),
            pltpu.VMEM((4, TERMS, LANES), f32),
            pltpu.VMEM((2, 8, LANES), f32),
            pltpu.VMEM((2, ROWS, LANES), f32),
            pltpu.VMEM((2, 8, LANES), f32),
            pltpu.VMEM((WIDE + 2 * SWEEPS + 1, ROWS, LANES), f32),
            pltpu.VMEM((4, 8, LANES), f32),
            pltpu.VMEM((4, 6, 8, LANES), f32),
            pltpu.VMEM((2, WIDE + 2 * SWEEPS + 1, ROWS, LANES), f32),
            pltpu.VMEM((WIDE + 2 * SWEEPS + 1, ROWS, LANES), f32),
            pltpu.SemaphoreType.DMA((5,)),
            pltpu.SemaphoreType.DMA((2 * RING,)),
            pltpu.SemaphoreType.DMA((4,)),
            pltpu.SemaphoreType.DMA((4,)),
            pltpu.SemaphoreType.DMA((8,)),
            pltpu.SemaphoreType.DMA((8,)),
            pltpu.SemaphoreType.DMA((4,)),
            pltpu.SemaphoreType.DMA((4,)),
            pltpu.SemaphoreType.DMA((len(PLACE),)),
            pltpu.SemaphoreType.DMA((len(PLACE),)),
            pltpu.SemaphoreType.DMA((len(CROSS) + 2,)),
            pltpu.SemaphoreType.DMA((len(CROSS) + 2,)),
            pltpu.SemaphoreType.DMA((4, 8)),
            pltpu.SemaphoreType.DMA((4, 8)),
        ],
        compiler_params=pltpu.CompilerParams(
            collective_id=0, has_side_effects=True, vmem_limit_bytes=48000 * 1024
        ),
        name="galerkin_step",
    )(
        *(
            pltpu.with_memory_space_constraint(value, pltpu.HBM)
            for value in (
                start_field.reshape(modes * wide, lanes),
                right_side.reshape(modes * wide, lanes),
                mean_coef,
                term_coef.reshape(-1, lanes),
                coupling,
                block_mask,
            )
        )
    )
    hbm = pl.BlockSpec(memory_space=pltpu.HBM)
    sol, res = pl.pallas_call(
        place,
        out_shape=(flat, flat),
        in_specs=[vmem, vmem],
        out_specs=(hbm, hbm),
        scratch_shapes=[pltpu.SemaphoreType.DMA((2,))],
        compiler_params=pltpu.CompilerParams(vmem_limit_bytes=1 << 20),
        name="place",
    )(sol, res)
    return (sol.reshape(start_field.shape), res.reshape(start_field.shape))


def solution(mesh):
    placed = (
        P("mode", "sx", "sy"),
        P("mode", "sx", "sy"),
        P("sx", "sy"),
        P(None, "sx", "sy"),
        P(None, None, "mode"),
        P(),
    )
    return jax.shard_map(
        local,
        mesh=mesh,
        in_specs=placed,
        out_specs=(P("mode", "sx", "sy"), P("mode", "sx", "sy")),
        check_vma=False,
    )
```
